256 devices in a mesh: seq: 64 (over z, x, core), kvh: 4 (over y).
Axes of the slice: x: 4, y: 4, z: 8, core: 2. Of those that a mesh axis runs over, the one named last changes fastest.
Arguments:
- queries: bfloat16 [8192, 28, 128], P('seq', 'kvh'), may hold values from -80 to 80
- new_keys: bfloat16 [8192, 4, 128], P('seq', 'kvh'), may hold values from -8 to 8
- cache_keys: bfloat16 [4096, 4, 128], P('seq', 'kvh'), may hold values from -1.1953125 to 1.1953125
- window_start: int32 [64], replicated, may hold values from 0 to 7680, as said below
- owner_slot: int32 [64], replicated, may hold values from 0 to 4095, as said below
Outputs:
- relevance: bfloat16 [8192, 28, 4096], P('seq', 'kvh')
- rep_bank: bfloat16 [4096, 4, 128], P('seq', 'kvh')
The draws below stay inside these ranges and needn't reach their ends.
Inputs may be any that keep to these rules, and one draw needn't show every extreme that they name: `window_start`: each window lies inside the new tokens; some window begins at the first new token and some ends at the last. `owner_slot`: the slots are distinct; the first and the last memory block are always among them.
All inputs are finite; a program needn't handle non-finite values.
Results may differ from the reference program's by a relative error of at most 0.0018.
Values may be sent and summed in bfloat16 or wider, within the bound.
A program may use at most 64 MiB of HBM per device.

```python
import math
import jax
import jax.numpy as jnp
from jax import lax

HEADS = 28
KVH = 4
HD = 128
BLK = 128
WIN = 512
QTOK = 8192
NEWB = 64
CACHEB = 4096


def joint_draw(key):
    key_query = jax.random.fold_in(key, 11)
    key_keys = jax.random.fold_in(key, 12)
    key_window = jax.random.fold_in(key, 13)
    key_ends = jax.random.fold_in(key, 16)
    starts = jax.random.randint(key_window, (NEWB,), 0, QTOK - WIN + 1).astype(jnp.int32)
    end_keys = jax.random.split(key_ends, 2)
    first_pick = jax.random.randint(end_keys[0], (), 0, NEWB).astype(jnp.int32)
    second_pick = ((first_pick + 1 + jax.random.randint(end_keys[1], (), 0, NEWB - 1)) % NEWB).astype(jnp.int32)
    starts = starts.at[first_pick].set(jnp.int32(0))
    starts = starts.at[second_pick].set(jnp.int32(QTOK - WIN))
    key_rows = jnp.clip(jax.random.normal(key_keys, (QTOK, KVH, HD), jnp.float32), -8.0, 8.0)
    query_rows = jnp.clip(jax.random.normal(key_query, (QTOK, HEADS, HD), jnp.float32), -8.0, 8.0)
    return (query_rows, key_rows, starts)


def draw_queries(key, part):
    return joint_draw(key)[0].astype(jnp.bfloat16)


def draw_new_keys(key, part):
    return joint_draw(key)[1].astype(jnp.bfloat16)


def draw_window_start(key, part):
    return joint_draw(key)[2]


def draw_owner_slot(key, part):
    inner = jax.random.permutation(jax.random.fold_in(key, 21), CACHEB - 2)[:NEWB - 2].astype(jnp.int32) + 1
    ends = jnp.array([0, CACHEB - 1], dtype=jnp.int32)
    slots = jnp.concatenate([ends, inner])
    order = jax.random.permutation(jax.random.fold_in(key, 22), NEWB)
    return slots[order].astype(jnp.int32)


def block_scale(key, extent, cuts, low, largest):
    level, own = 1.0, jax.random.fold_in(key, 6)
    for position, shards_of in cuts:
        draws = jnp.exp(jax.random.uniform(jax.random.fold_in(own, position), (shards_of,), jnp.float32, low / len(cuts), largest / len(cuts)))
        level = level * jnp.repeat(draws, extent[position] // shards_of).reshape([-1 if axis == position else 1 for axis in range(len(extent))])
    return level


def normal_values(rng, shape, deviation, reach, pieces=(), held_as=jnp.bfloat16):
    level = block_scale(rng, shape, pieces, -0.22, 0.18) if pieces else 1.0
    values = jax.random.normal(rng, shape, jnp.float32) * deviation * level
    return jnp.minimum(jnp.maximum(values, -reach), reach).astype(held_as)


def setup_inputs(seed: int = 0) -> dict:
    key_list = jax.random.split(jax.random.key(seed), 6)
    queries = draw_queries(jax.random.fold_in(key_list[5], 71), 0)
    new_keys = draw_new_keys(jax.random.fold_in(key_list[5], 71), 0)
    cache_keys = normal_values(key_list[2], (CACHEB, KVH, HD), 0.15, 1.1953125, ((0, 64), (1, 4)))
    window_start = draw_window_start(jax.random.fold_in(key_list[5], 71), 0)
    owner_slot = draw_owner_slot(jax.random.fold_in(key_list[5], 71), 0)
    return {"queries": queries, "new_keys": new_keys, "cache_keys": cache_keys, "window_start": window_start, "owner_slot": owner_slot}


def reference(queries, new_keys, cache_keys, window_start, owner_slot):
    group_size = HEADS // KVH
    score_scale = 1.0 / math.sqrt(HD)

    def one_block(block_index):
        begin = window_start[block_index].astype(jnp.int32)
        window_q = lax.dynamic_slice_in_dim(queries, begin, WIN, 0).astype(jnp.float32)
        window_q = window_q.reshape(WIN, KVH, group_size, HD)
        block_keys = lax.dynamic_slice_in_dim(new_keys, (block_index * BLK).astype(jnp.int32), BLK, 0).astype(jnp.float32)
        scores = jnp.einsum('wgjd,kgd->wgjk', window_q, block_keys, precision=lax.Precision.HIGHEST) * score_scale
        softmax_weights = jax.nn.softmax(scores, axis=-1)
        weights = lax.optimization_barrier(jnp.sum(softmax_weights, axis=(0, 2))) / (group_size * WIN)
        merged = jnp.einsum('gk,kgd->gd', weights, block_keys, precision=lax.Precision.HIGHEST)
        return merged.astype(jnp.bfloat16)
    representative = lax.map(one_block, jnp.arange(NEWB, dtype=jnp.int32))
    key_bank = cache_keys.at[owner_slot].set(representative)
    query_block = math.gcd(QTOK, 512)
    bank_float = key_bank.astype(jnp.float32)

    def score_block(query_part):
        grouped = query_part.astype(jnp.float32).reshape(query_block, KVH, group_size, HD)
        result = jnp.einsum('tgjd,bgd->tgjb', grouped, bank_float) * score_scale
        return result.astype(jnp.bfloat16).reshape(query_block, HEADS, CACHEB)
    relevance = lax.map(score_block, queries.reshape(QTOK // query_block, query_block, HEADS, HD))
    return (relevance.reshape(QTOK, HEADS, CACHEB), key_bank)
```

```python
import functools
import math

import jax
import jax.numpy as jnp
from jax import lax
from jax.experimental import pallas as pl
from jax.experimental.pallas import tpu as pltpu
from jax.sharding import PartitionSpec as P

BLK = 128
WIN = 512
NX = 4
HEAD_CUT = 4
MESH = pl.DeviceIdType.MESH
VMEM = pltpu.VMEM


def refresh_kernel(
    nz, ws, q_hbm, k_hbm, b_hbm, bank_out, rep_out,
    qb, kb, bb, acc, pb, rb, rx,
    lsem, ksend, krecv, dsend, drecv, qsend, qrecv, bsend, brecv,
    cs, cr, es, er, ps, pr, xs, xr, osem,
):
    group, tok, hd = q_hbm.shape
    half_z = nz // 2
    groups = nz // 2
    s = lax.axis_index("seq")
    z, x, c = s // (2 * NX), (s // 2) % NX, s % 2
    xc = x * 2 + c
    exp_scale = math.log2(math.e) / math.sqrt(hd)

    def dev(zz, xx, cc):
        return {"seq": (lax.rem(zz, nz) * NX + lax.rem(xx, NX)) * 2 + cc}

    def remote(src, dst, ssem, rsem, target):
        return pltpu.make_async_remote_copy(
            src_ref=src, dst_ref=dst, send_sem=ssem, recv_sem=rsem,
            device_id=target, device_id_type=MESH,
        )

    sibling = dev(z, x, 1 - c)
    east, west = dev(z, x + 1, c), dev(z, x + NX - 1, c)

    own = [
        pltpu.make_async_copy(k_hbm, kb.at[0, 0], lsem.at[0]),
        pltpu.make_async_copy(q_hbm, qb.at[0], lsem.at[1]),
        pltpu.make_async_copy(b_hbm, bb.at[z, xc], lsem.at[2]),
    ]
    for copy in own:
        copy.start()

    peers = [dev(z + dz, x, (c + dc) % 2) for dz in range(nz) for dc in range(2) if dz or dc]
    peers += [dev(z, x + dx, (c + dc) % 2) for dx in range(1, NX) for dc in range(2)]
    barrier = pltpu.get_barrier_semaphore()
    for peer in peers:
        pl.semaphore_signal(barrier, inc=1, device_id=peer, device_id_type=MESH)
    acc[...] = jnp.zeros_like(acc)
    pl.semaphore_wait(barrier, len(peers))

    key_z = {d: remote(kb.at[0, 0], kb.at[d, 0], ksend.at[d], krecv.at[d], dev(z + d, x, c)) for d in range(1, nz)}
    key_core = {d: remote(kb.at[d, 0], kb.at[d, 1], dsend.at[d], drecv.at[d], sibling) for d in range(nz)}
    lo, hi = pl.ds(0, HEAD_CUT), pl.ds(HEAD_CUT, group - HEAD_CUT)

    def q_copy(i, src_slot, dst_slot, heads, target):
        return remote(qb.at[src_slot, heads], qb.at[dst_slot, heads], qsend.at[i], qrecv.at[i], target)

    q_x = [
        q_copy(0, 0, 1, lo, east), q_copy(1, 0, 1, hi, east),
        q_copy(2, 0, 3, hi, west), q_copy(3, 0, 3, lo, west),
        q_copy(4, 1, 2, lo, east), q_copy(5, 3, 2, hi, west),
    ]
    bank_z = {d: remote(bb.at[z, xc], bb.at[z, xc], bsend.at[d], brecv.at[d], dev(z + d, x, c)) for d in range(1, nz)}
    first, last = pl.ds(0, half_z), pl.ds(half_z, half_z)

    def c_copy(i, column, rows, target):
        return remote(bb.at[rows, column], bb.at[rows, column], cs.at[i], cr.at[i], target)

    def column(dx):
        return lax.rem(x + dx, NX) * 2 + c

    west_of, east_of = column(NX - 1), column(1)
    bank_x = [
        c_copy(0, xc, first, east), c_copy(1, xc, last, east),
        c_copy(2, xc, last, west), c_copy(3, xc, first, west),
        c_copy(4, west_of, first, east), c_copy(5, east_of, last, west),
    ]
    bank_in = [
        c_copy(0, west_of, first, east), c_copy(1, west_of, last, east),
        c_copy(2, east_of, last, west), c_copy(3, east_of, first, west),
        c_copy(4, column(2), first, east), c_copy(5, column(2), last, west),
    ]

    def e_copy(dx):
        return remote(bb.at[:, column(dx)], bb.at[:, column(dx)], es.at[dx], er.at[dx], sibling)

    bank_core = [e_copy(dx) for dx in range(NX)]

    def start_all():
        own[0].wait()
        key_core[0].start()
        order = sorted(range(1, nz), key=lambda d: (min(d, nz - d), d))
        for d in order:
            key_z[d].start()
        own[1].wait()
        for i in (0, 2, 1, 3):
            q_x[i].start()
        own[2].wait()
        for d in order:
            bank_z[d].start()

    def forward_key(*offsets):
        for d in offsets:
            key_z[d].wait_recv()
            key_core[d].start()

    def have_keys(*offsets):
        for d in offsets:
            key_core[d].wait_recv()

    def forward_queries():
        q_x[0].wait_recv()
        q_x[4].start()
        q_x[2].wait_recv()
        q_x[5].start()

    def bank_rows():
        for d in range(1, nz):
            bank_z[d].wait_recv()
        for i in (0, 2, 1, 3):
            bank_x[i].start()
        bank_core[0].start()

    def bank_forward():
        bank_in[0].wait_recv()
        bank_x[4].start()
        bank_in[2].wait_recv()
        bank_x[5].start()

    def bank_cross():
        bank_in[1].wait_recv()
        bank_core[3].start()
        bank_in[3].wait_recv()
        bank_core[1].start()

    def at_step(step):
        tile, g = step // groups, step % groups
        if step == 0:
            start_all()
        if tile == 0:
            near = [d for d in {g + 1, (nz - g) % nz} if d]
            forward_key(*near)
            if g == min(1, groups - 1):
                forward_queries()
            have_keys(*sorted({g + 1, (nz - g) % nz}))
        if tile == 1 and g == 0:
            q_x[1].wait_recv()
            bank_rows()
        if tile == 2 and g == 0:
            q_x[3].wait_recv()
        if tile == 2 and g == groups - 1:
            bank_forward()
        if tile == 3 and g == 0:
            q_x[4].wait_recv()
            q_x[5].wait_recv()

    lane = lax.broadcasted_iota(jnp.int32, (1, BLK), 1)

    def compute(step):
        tile, g = step // groups, step % groups
        slot = tile ^ (tile >> 1)
        base = (z * 2 * NX + lax.rem(x - slot + NX, NX) * 2 + c) * tok
        position = base + lane
        offsets = [lax.rem(nz - g, nz), g + 1]
        members = [(d, rel) for d in offsets for rel in range(2)]
        keys = jnp.concatenate([kb[d].reshape(2 * BLK, hd) for d in offsets], axis=0)
        inside = []
        for d, rel in members:
            block = (lax.rem(z - d + nz, nz) * NX + x) * 2 + (c + rel) % 2
            begin = ws[block]
            inside.append(((position >= begin) & (position < begin + WIN)).astype(jnp.float32))
        sums = [acc[d, rel] for d, rel in members]
        for h in range(0, group, 2):
            heads = min(2, group - h)
            rows = qb[slot, pl.ds(h, heads)].reshape(heads * tok, hd)
            scores = lax.dot_general(
                keys, rows, (((1,), (1,)), ((), ())), preferred_element_type=jnp.float32
            )
            for i in range(len(members)):
                part = scores[i * BLK : (i + 1) * BLK]
                top = jnp.max(part, axis=0, keepdims=True)
                e = jnp.exp2((part - top) * exp_scale)
                total = jnp.sum(e, axis=0, keepdims=True)
                for j in range(heads):
                    cut = slice(j * tok, (j + 1) * tok)
                    sums[i] = sums[i] + e[:, cut] * (inside[i] / total[:, cut])
        for (d, rel), value in zip(members, sums):
            acc[d, rel] = value

    @pl.loop(0, NX * groups)
    def _(step):
        for k in range(NX * groups):
            pl.when(step == k)(functools.partial(at_step, k))
        compute(step)

    for d in range(nz):
        for rel in range(2):
            weight = jnp.sum(acc[d, rel], axis=1, keepdims=True)
            row = jnp.sum(weight * kb[d, rel].astype(jnp.float32), axis=0, keepdims=True)
            pb[(c + rel) % 2, pl.ds(lax.rem(z - d + nz, nz), 1), :] = row

    column_peers = [(dz, dc) for dz in range(nz) for dc in range(2) if dz or dc]
    parts = [
        remote(pb.at[(c + dc) % 2], rb.at[dz * 2 + dc], ps.at[dz * 2 + dc], pr.at[dz * 2 + dc], dev(z + dz, x, (c + dc) % 2))
        for dz, dc in column_peers
    ]
    for copy in parts:
        copy.start()
    rb[0] = pb[c]
    bank_cross()
    for copy in parts:
        copy.wait_recv()
    total = jnp.zeros((nz, hd), jnp.float32)
    for dz in range(nz):
        for dc in range(2):
            total = total + rb[lax.rem(z - dz + nz, nz) * 2 + (c + dc) % 2]
    mine = pl.ds(pl.multiple_of(xc * nz, nz), nz)
    rx[mine, :] = total / (group * WIN)
    row_peers = [(dx, dc) for dx in range(NX) for dc in range(2) if dx or dc]
    sums_x = [
        remote(rx.at[mine], rx.at[mine], xs.at[dx * 2 + dc], xr.at[dx * 2 + dc], dev(z, x + dx, (c + dc) % 2))
        for dx, dc in row_peers
    ]
    for copy in sums_x:
        copy.start()
    bank_in[4].wait_recv()
    bank_in[5].wait_recv()
    bank_core[2].start()
    for copy in bank_core:
        copy.wait_recv()
    bank_done = pltpu.make_async_copy(bb, bank_out, osem.at[0])
    bank_done.start()
    for copy in sums_x:
        copy.wait_recv()
    for zz in range(0, nz, 2):
        pair = [rx[pl.ds(zz + i, 2 * NX, stride=nz), :] for i in range(2)]
        rep_out[pl.ds(zz * 2 * NX, 4 * NX), :] = jnp.concatenate(pair, axis=0).astype(jnp.bfloat16)
    for copy in [*key_z.values(), *key_core.values(), *q_x, *bank_z.values(), *bank_x, *bank_core, *parts, *sums_x]:
        copy.wait_send()
    bank_done.wait()


def refresh(nz, window_start, q, k, b):
    group, tok, hd = q.shape
    hbm = pl.BlockSpec(memory_space=pl.ANY)
    dma = pltpu.SemaphoreType.DMA
    bank_shape = (nz, 2 * NX, *b.shape)
    return pl.pallas_call(
        functools.partial(refresh_kernel, nz),
        out_shape=(
            jax.ShapeDtypeStruct(bank_shape, jnp.bfloat16),
            jax.ShapeDtypeStruct((nz * 2 * NX, hd), jnp.bfloat16),
        ),
        in_specs=[pl.BlockSpec(memory_space=pltpu.SMEM), hbm, hbm, hbm],
        out_specs=(hbm, pl.BlockSpec(memory_space=VMEM)),
        scratch_shapes=[
            VMEM((NX, group, tok, hd), jnp.bfloat16),
            VMEM((nz, 2, BLK, hd), jnp.bfloat16),
            VMEM(bank_shape, jnp.bfloat16),
            VMEM((nz, 2, BLK, BLK), jnp.float32),
            VMEM((2, nz, hd), jnp.float32),
            VMEM((2 * nz, nz, hd), jnp.float32),
            VMEM((2 * NX * nz, hd), jnp.float32),
            dma((3,)),
            dma((nz,)), dma((nz,)), dma((nz,)), dma((nz,)),
            dma((6,)), dma((6,)),
            dma((nz,)), dma((nz,)),
            dma((6,)), dma((6,)), dma((NX,)), dma((NX,)),
            dma((2 * nz,)), dma((2 * nz,)), dma((2 * NX,)), dma((2 * NX,)),
            dma((1,)),
        ],
        compiler_params=pltpu.CompilerParams(collective_id=0, has_side_effects=True),
        name="refresh",
    )(window_start, q, k, b)


def patched(slots, first_row, reps, rows):
    count = rows.shape[0]
    row = first_row + lax.broadcasted_iota(jnp.int32, (count, slots.shape[1]), 0)
    chosen = (row == slots).astype(jnp.bfloat16)
    both = jnp.concatenate([reps, jnp.ones_like(reps)], axis=1)
    placed = jnp.dot(chosen, both, preferred_element_type=jnp.float32)
    hd = reps.shape[1]
    return jnp.where(placed[:, hd:] > 0.5, placed[:, :hd], rows.astype(jnp.float32)).astype(jnp.bfloat16)


def relevance_kernel(slots, q, bank, reps, shard, out, shard_out):
    step = pl.program_id(0)
    width = bank.shape[0]
    tile = patched(slots[...], step * width, reps[...], bank[...])
    scores = lax.dot_general(q[...], tile, (((1,), (1,)), ((), ())), preferred_element_type=jnp.float32)
    out[...] = (scores * (1.0 / math.sqrt(q.shape[1]))).astype(jnp.bfloat16)

    @pl.when(step == 0)
    def _():
        first_row = lax.axis_index("seq") * shard.shape[0]
        shard_out[...] = patched(slots[...], first_row, reps[...], shard[...])


def relevance_of(slots, q, bank, reps, shard, tile=512):
    rows, hd = q.shape
    total = bank.shape[0]

    def whole(array):
        return pl.BlockSpec(array.shape, lambda i: (0, 0))

    return pl.pallas_call(
        relevance_kernel,
        grid=(total // tile,),
        out_shape=(
            jax.ShapeDtypeStruct((rows, total), jnp.bfloat16),
            jax.ShapeDtypeStruct(shard.shape, jnp.bfloat16),
        ),
        in_specs=[whole(slots), whole(q), pl.BlockSpec((tile, hd), lambda i: (i, 0)), whole(reps), whole(shard)],
        out_specs=(pl.BlockSpec((rows, tile), lambda i: (0, i)), whole(shard)),
        compiler_params=pltpu.CompilerParams(dimension_semantics=("arbitrary",)),
        name="relevance",
    )(slots, q, bank, reps, shard)


def per_device(nz, queries, new_keys, cache_keys, window_start, owner_slot):
    tok, group, hd = queries.shape
    q = queries.transpose(1, 0, 2)
    shard = cache_keys[:, 0, :]
    bank, reps = refresh(nz, window_start, q, new_keys[:, 0, :], shard)
    total = nz * 2 * NX * shard.shape[0]
    relevance, new_shard = relevance_of(
        owner_slot.reshape(1, -1), q.reshape(group * tok, hd), bank.reshape(total, hd), reps, shard
    )
    relevance = relevance.reshape(group, tok, total).transpose(1, 0, 2)
    return (relevance, new_shard[:, None, :])


def solution(mesh):
    nz = mesh.shape["seq"] // (2 * NX)
    split = P("seq", "kvh", None)
    return jax.shard_map(
        functools.partial(per_device, nz),
        mesh=mesh,
        in_specs=(split, split, split, P(), P()),
        out_specs=(split, split),
        check_vma=False,
    )
```

```python
import functools
import math

import jax
import jax.numpy as jnp
from jax import lax
from jax.experimental import pallas as pl
from jax.experimental.pallas import tpu as pltpu
from jax.sharding import PartitionSpec as P

BLK = 128
WIN = 512
NX = 4
HEAD_CUT = 4
MESH = pl.DeviceIdType.MESH
VMEM = pltpu.VMEM


def on_chip(shape, dtype):
    return VMEM(shape, dtype)


def kept(array):
    return pltpu.with_memory_space_constraint(array, VMEM)


def refresh_kernel(
    nz, ws, slots, q_hbm, k_hbm, b_hbm, rhs_out, lhs_out, shard_out,
    qb, kb, bb, acc, pb, rb, rx,
    lsem, ksend, krecv, dsend, drecv, qsend, qrecv, bsend, brecv,
    cs, cr, es, er, ps, pr, xs, xr,
):
    group, tok, hd = q_hbm.shape
    half_z = nz // 2
    per = min(4, nz)
    groups = nz // per
    s = lax.axis_index("seq")
    z, x, c = s // (2 * NX), (s // 2) % NX, s % 2
    xc = x * 2 + c
    exp_scale = math.log2(math.e) / math.sqrt(hd)

    def dev(zz, xx, cc):
        return {"seq": (lax.rem(zz, nz) * NX + lax.rem(xx, NX)) * 2 + cc}

    def remote(src, dst, ssem, rsem, target):
        return pltpu.make_async_remote_copy(
            src_ref=src, dst_ref=dst, send_sem=ssem, recv_sem=rsem,
            device_id=target, device_id_type=MESH,
        )

    sibling = dev(z, x, 1 - c)
    east, west = dev(z, x + 1, c), dev(z, x + NX - 1, c)

    own = [
        pltpu.make_async_copy(k_hbm, kb.at[0, 0], lsem.at[0]),
        pltpu.make_async_copy(q_hbm, qb.at[0], lsem.at[1]),
        pltpu.make_async_copy(b_hbm, bb.at[z, xc], lsem.at[2]),
    ]
    for copy in own:
        copy.start()

    peers = [dev(z + dz, x, (c + dc) % 2) for dz in range(nz) for dc in range(2) if dz or dc]
    peers += [dev(z, x + dx, (c + dc) % 2) for dx in range(1, NX) for dc in range(2)]
    barrier = pltpu.get_barrier_semaphore()
    for peer in peers:
        pl.semaphore_signal(barrier, inc=1, device_id=peer, device_id_type=MESH)
    acc[...] = jnp.zeros_like(acc)
    pl.semaphore_wait(barrier, len(peers))

    key_z = {d: remote(kb.at[0, 0], kb.at[d, 0], ksend.at[d], krecv.at[d], dev(z + d, x, c)) for d in range(1, nz)}
    key_core = {d: remote(kb.at[d, 0], kb.at[d, 1], dsend.at[d], drecv.at[d], sibling) for d in range(nz)}
    lo, hi = pl.ds(0, HEAD_CUT), pl.ds(HEAD_CUT, group - HEAD_CUT)

    def q_copy(i, src_slot, dst_slot, heads, target):
        return remote(qb.at[src_slot, heads], qb.at[dst_slot, heads], qsend.at[i], qrecv.at[i], target)

    q_x = [
        q_copy(0, 0, 1, lo, east), q_copy(1, 0, 1, hi, east),
        q_copy(2, 0, 3, hi, west), q_copy(3, 0, 3, lo, west),
        q_copy(4, 1, 2, lo, east), q_copy(5, 3, 2, hi, west),
    ]
    bank_z = {d: remote(bb.at[z, xc], bb.at[z, xc], bsend.at[d], brecv.at[d], dev(z + d, x, c)) for d in range(1, nz)}
    first, last = pl.ds(0, half_z), pl.ds(half_z, half_z)

    def c_copy(i, column, rows, target):
        return remote(bb.at[rows, column], bb.at[rows, column], cs.at[i], cr.at[i], target)

    def column(dx):
        return lax.rem(x + dx, NX) * 2 + c

    west_of, east_of = column(NX - 1), column(1)
    bank_x = [
        c_copy(0, xc, first, east), c_copy(1, xc, last, east),
        c_copy(2, xc, last, west), c_copy(3, xc, first, west),
        c_copy(4, west_of, first, east), c_copy(5, east_of, last, west),
    ]
    bank_in = [
        c_copy(0, west_of, first, east), c_copy(1, west_of, last, east),
        c_copy(2, east_of, last, west), c_copy(3, east_of, first, west),
        c_copy(4, column(2), first, east), c_copy(5, column(2), last, west),
    ]

    def e_copy(dx):
        return remote(bb.at[:, column(dx)], bb.at[:, column(dx)], es.at[dx], er.at[dx], sibling)

    bank_core = [e_copy(dx) for dx in range(NX)]

    near = [0, 1, nz - 1, 2][:per]

    def start_all():
        own[0].wait()
        key_core[0].start()
        for d in sorted(range(1, nz), key=lambda d: (min(d, nz - d), d)):
            key_z[d].start()
        own[1].wait()
        for i in (0, 2, 1, 3):
            q_x[i].start()
        lhs_out[:, :hd] = qb[0].reshape(group * tok, hd)

    def forward_key(*offsets):
        for d in offsets:
            if d in key_z:
                key_z[d].wait_recv()
                key_core[d].start()

    def have_keys(offsets):
        for d in offsets:
            key_core[d].wait_recv()

    def forward_queries():
        q_x[0].wait_recv()
        q_x[4].start()
        q_x[2].wait_recv()
        q_x[5].start()

    def bank_rows():
        for d in range(1, nz):
            bank_z[d].wait_recv()
        for i in (0, 2, 1, 3):
            bank_x[i].start()
        bank_core[0].start()

    def bank_forward():
        bank_in[0].wait_recv()
        bank_x[4].start()
        bank_in[2].wait_recv()
        bank_x[5].start()

    def bank_cross():
        bank_in[1].wait_recv()
        bank_core[3].start()
        bank_in[3].wait_recv()
        bank_core[1].start()

    def at_step(step):
        pair, g = step // groups, step % groups
        if step == 0:
            start_all()
            forward_key(1)
            if nz > 2:
                forward_key(nz - 1, 2)
            forward_queries()
            own[2].wait()
            for d in range(1, nz):
                bank_z[d].start()
            if nz > 4:
                forward_key(nz - 2)
            have_keys(near)
            q_x[1].wait_recv()
            q_x[3].wait_recv()
        if pair == 0 and g == 1:
            forward_key(3, nz - 3, 4)
            have_keys([d for d in range(nz) if d not in near])
        if pair == 1 and g == 0:
            bank_rows()
            q_x[4].wait_recv()
            q_x[5].wait_recv()

    lane = lax.broadcasted_iota(jnp.int32, (1, BLK), 1)

    def compute(step):
        pair, g = step // groups, step % groups
        tiles = (1 - pair, 3 - pair)
        offsets = near if groups == 1 else [6 * g, 1 + 2 * g, 7 - 2 * g, 2 + 2 * g]
        members = [(d, rel) for d in offsets for rel in range(2)]
        keys = jnp.concatenate([kb[d].reshape(2 * BLK, hd) for d in offsets], axis=0)
        position = [(z * 2 * NX + lax.rem(x - t + NX, NX) * 2 + c) * tok + lane for t in tiles]
        first_in, any_in = [], []
        for d, rel in members:
            begin = ws[(lax.rem(z - d + nz, nz) * NX + x) * 2 + (c + rel) % 2]
            hit = [(p >= begin) & (p < begin + WIN) for p in position]
            first_in.append(hit[0])
            any_in.append((hit[0] | hit[1]).astype(jnp.float32))
        sums = [acc[d, rel] for d, rel in members]
        for h in range(group):
            rows = jnp.concatenate([qb[t, h] for t in tiles], axis=0)
            scores = lax.dot_general(
                keys, rows, (((1,), (1,)), ((), ())), preferred_element_type=jnp.float32
            )
            for i in range(len(members)):
                both = scores[i * BLK : (i + 1) * BLK]
                part = jnp.where(first_in[i], both[:, :tok], both[:, tok:])
                top = jnp.max(part, axis=0, keepdims=True)
                e = jnp.exp2((part - top) * exp_scale)
                sums[i] = sums[i] + e * (any_in[i] / jnp.sum(e, axis=0, keepdims=True))
        for (d, rel), value in zip(members, sums):
            acc[d, rel] = value

    @pl.loop(0, 2 * groups)
    def _(step):
        for k in range(2 * groups):
            pl.when(step == k)(functools.partial(at_step, k))
        compute(step)

    for d in range(nz):
        for rel in range(2):
            weight = jnp.sum(acc[d, rel], axis=1, keepdims=True)
            row = jnp.sum(weight * kb[d, rel].astype(jnp.float32), axis=0, keepdims=True)
            pb[(c + rel) % 2, pl.ds(lax.rem(z - d + nz, nz), 1), :] = row

    column_peers = [(dz, dc) for dz in range(nz) for dc in range(2) if dz or dc]
    parts = [
        remote(pb.at[(c + dc) % 2], rb.at[dz * 2 + dc], ps.at[dz * 2 + dc], pr.at[dz * 2 + dc], dev(z + dz, x, (c + dc) % 2))
        for dz, dc in column_peers
    ]
    for copy in parts:
        copy.start()
    rb[0] = pb[c]
    bank_forward()
    bank_cross()
    for copy in parts:
        copy.wait_recv()
    total = jnp.zeros((nz, hd), jnp.float32)
    for dz in range(nz):
        for dc in range(2):
            total = total + rb[lax.rem(z - dz + nz, nz) * 2 + (c + dc) % 2]
    mine = pl.ds(pl.multiple_of(xc * nz, nz), nz)
    rx[mine, :] = total / (group * WIN)
    row_peers = [(dx, dc) for dx in range(NX) for dc in range(2) if dx or dc]
    sums_x = [
        remote(rx.at[mine], rx.at[mine], xs.at[dx * 2 + dc], xr.at[dx * 2 + dc], dev(z, x + dx, (c + dc) % 2))
        for dx, dc in row_peers
    ]
    for copy in sums_x:
        copy.start()
    bank_in[4].wait_recv()
    bank_in[5].wait_recv()
    bank_core[2].start()
    for copy in bank_core:
        copy.wait_recv()
    columns = jnp.concatenate([slots[...], slots[...]], axis=1)
    width = 2 * NX * b_hbm.shape[0]

    def hits(first_row, count):
        row = first_row + lax.broadcasted_iota(jnp.int32, (count, columns.shape[1]), 0)
        chosen = (row == columns).astype(jnp.float32)
        return chosen, jnp.max(chosen, axis=1, keepdims=True) > 0.5

    @pl.loop(0, nz)
    def _(zz):
        start = pl.multiple_of(zz * width, width)
        chosen, taken = hits(start, width)
        rest = jnp.where(taken, 0.0, bb[zz].reshape(width, hd).astype(jnp.float32))
        rhs_out[pl.ds(start, width), :] = jnp.concatenate([rest, chosen], axis=1).astype(jnp.bfloat16)

    for copy in sums_x:
        copy.wait_recv()
    ordered = [rx[pl.ds(zz, 2 * NX, stride=nz), :] for zz in range(nz)]
    reps = jnp.concatenate(ordered, axis=0).astype(jnp.bfloat16)
    value = lax.dot_general(
        lhs_out[:, :hd], reps, (((1,), (1,)), ((), ())), preferred_element_type=jnp.float32
    )
    high = value.astype(jnp.bfloat16)
    low = (value - high.astype(jnp.float32)).astype(jnp.bfloat16)
    lhs_out[:, hd:] = jnp.concatenate([high, low], axis=1)
    held = b_hbm.shape[0]
    chosen, taken = hits(s * held, held)
    placed = jnp.dot(
        chosen[:, : reps.shape[0]].astype(jnp.bfloat16), reps, preferred_element_type=jnp.float32
    )
    shard_out[...] = jnp.where(taken, placed, bb[z, xc].astype(jnp.float32)).astype(jnp.bfloat16)
    for copy in [*key_z.values(), *key_core.values(), *q_x, *bank_z.values(), *bank_x, *bank_core, *parts, *sums_x]:
        copy.wait_send()


def refresh(nz, window_start, slots, q, k, b):
    group, tok, hd = q.shape
    hbm = pl.BlockSpec(memory_space=pl.ANY)
    vmem = pl.BlockSpec(memory_space=VMEM)
    dma = pltpu.SemaphoreType.DMA
    bank_shape = (nz, 2 * NX, *b.shape)
    return pl.pallas_call(
        functools.partial(refresh_kernel, nz),
        out_shape=(
            on_chip((nz * 2 * NX * b.shape[0], hd + 2 * slots.shape[1]), jnp.bfloat16),
            on_chip((group * tok, hd + 2 * slots.shape[1]), jnp.bfloat16),
            on_chip(b.shape, jnp.bfloat16),
        ),
        in_specs=[pl.BlockSpec(memory_space=pltpu.SMEM), vmem, hbm, hbm, hbm],
        out_specs=(vmem, vmem, vmem),
        scratch_shapes=[
            VMEM((NX, group, tok, hd), jnp.bfloat16),
            VMEM((nz, 2, BLK, hd), jnp.bfloat16),
            VMEM(bank_shape, jnp.bfloat16),
            VMEM((nz, 2, BLK, BLK), jnp.float32),
            VMEM((2, nz, hd), jnp.float32),
            VMEM((2 * nz, nz, hd), jnp.float32),
            VMEM((2 * NX * nz, hd), jnp.float32),
            dma((3,)),
            dma((nz,)), dma((nz,)), dma((nz,)), dma((nz,)),
            dma((6,)), dma((6,)),
            dma((nz,)), dma((nz,)),
            dma((6,)), dma((6,)), dma((NX,)), dma((NX,)),
            dma((2 * nz,)), dma((2 * nz,)), dma((2 * NX,)), dma((2 * NX,)),
        ],
        compiler_params=pltpu.CompilerParams(collective_id=0, has_side_effects=True),
        name="refresh",
    )(window_start, slots, q, k, b)


def relevance_kernel(tile, lhs, rhs, shard, out, shard_out, held, sem):
    scale = 1.0 / math.sqrt(BLK)
    copies = [pltpu.make_async_copy(shard, shard_out, sem.at[0])]
    copies[0].start()
    for i in range(out.shape[1] // tile):
        cut = pl.ds(i * tile, tile)
        scores = lax.dot_general(
            lhs[...], rhs[cut, :], (((1,), (1,)), ((), ())), preferred_element_type=jnp.float32
        )
        held[:, cut] = (scores * scale).astype(jnp.bfloat16)
        copy = pltpu.make_async_copy(held.at[:, cut], out.at[:, cut], sem.at[i + 1])
        copy.start()
        copies.append(copy)
    for copy in copies:
        copy.wait()


def relevance_of(lhs, rhs, shard, tile=512):
    rows, total = lhs.shape[0], rhs.shape[0]
    vmem = pl.BlockSpec(memory_space=VMEM)
    hbm = pl.BlockSpec(memory_space=pl.ANY)
    lhs, rhs, shard = (kept(a) for a in (lhs, rhs, shard))
    return pl.pallas_call(
        functools.partial(relevance_kernel, tile),
        out_shape=(
            jax.ShapeDtypeStruct((rows, total), jnp.bfloat16),
            jax.ShapeDtypeStruct(shard.shape, jnp.bfloat16),
        ),
        in_specs=[vmem, vmem, vmem],
        out_specs=(hbm, hbm),
        scratch_shapes=[
            VMEM((rows, total), jnp.bfloat16),
            pltpu.SemaphoreType.DMA((1 + total // tile,)),
        ],
        name="relevance",
    )(lhs, rhs, shard)


def per_device(nz, queries, new_keys, cache_keys, window_start, owner_slot):
    tok, group, hd = queries.shape
    q = queries.transpose(1, 0, 2)
    rhs, lhs, shard = refresh(
        nz, window_start, owner_slot.reshape(1, -1), q, new_keys[:, 0, :], cache_keys[:, 0, :]
    )
    relevance, new_shard = relevance_of(lhs, rhs, shard)
    relevance = relevance.reshape(group, tok, rhs.shape[0]).transpose(1, 0, 2)
    return (relevance, new_shard[:, None, :])


def solution(mesh):
    nz = mesh.shape["seq"] // (2 * NX)
    split = P("seq", "kvh", None)
    return jax.shard_map(
        functools.partial(per_device, nz),
        mesh=mesh,
        in_specs=(split, split, split, P(), P()),
        out_specs=(split, split),
        check_vma=False,
    )
```

```python
import functools
import math

import jax
import jax.numpy as jnp
from jax import lax
from jax.experimental import pallas as pl
from jax.experimental.pallas import tpu as pltpu
from jax.sharding import PartitionSpec as P

BLK = 128
WIN = 512
NX = 4
HEAD_CUT = 4
MESH = pl.DeviceIdType.MESH
VMEM = pltpu.VMEM


def on_chip(shape, dtype):
    return VMEM(shape, dtype)


def kept(array):
    return pltpu.with_memory_space_constraint(array, VMEM)


def refresh_kernel(
    nz, ws_hbm, slots_hbm, q_hbm, k_hbm, b_hbm, rhs_out, lhs_out, shard_out,
    ws, slots, qb, kb, bb, keep, acc, pb, rb, rx,
    lsem, ksend, krecv, dsend, drecv, qsend, qrecv, bsend, brecv,
    cs, cr, es, er, ps, pr, xs, xr,
):
    group, tok, hd = q_hbm.shape
    held = b_hbm.shape[0]
    half_z = nz // 2
    per = min(4, nz)
    groups = nz // per
    s = lax.axis_index("seq")
    z, x, c = s // (2 * NX), (s // 2) % NX, s % 2
    xc = x * 2 + c
    exp_scale = math.log2(math.e) / math.sqrt(hd)

    def dev(zz, xx, cc):
        return {"seq": (lax.rem(zz, nz) * NX + lax.rem(xx, NX)) * 2 + cc}

    def remote(src, dst, ssem, rsem, target):
        return pltpu.make_async_remote_copy(
            src_ref=src, dst_ref=dst, send_sem=ssem, recv_sem=rsem,
            device_id=target, device_id_type=MESH,
        )

    sibling = dev(z, x, 1 - c)
    east, west = dev(z, x + 1, c), dev(z, x + NX - 1, c)

    own = [
        pltpu.make_async_copy(k_hbm, kb.at[0, 0], lsem.at[0]),
        pltpu.make_async_copy(q_hbm, qb.at[0], lsem.at[1]),
        pltpu.make_async_copy(b_hbm, bb.at[z, xc], lsem.at[2]),
        pltpu.make_async_copy(slots_hbm, slots, lsem.at[3]),
        pltpu.make_async_copy(ws_hbm, ws, lsem.at[4]),
    ]
    for copy in own:
        copy.start()

    direct = sorted({d % nz for d in (1, -1, 2, -2)} - {0}, key=lambda d: (min(d, nz - d), d))
    peers = [sibling, east, west] + [dev(z + d, x, c) for d in direct]
    barrier = pltpu.get_barrier_semaphore()
    for peer in peers:
        pl.semaphore_signal(barrier, inc=1, device_id=peer, device_id_type=MESH)

    pl.semaphore_wait(barrier, len(peers))

    width = 2 * NX * held

    def hits(first_row, count):
        columns = jnp.concatenate([slots[...], slots[...]], axis=1)
        row = first_row + lax.broadcasted_iota(jnp.int32, (count, columns.shape[1]), 0)
        chosen = (row == columns).astype(jnp.float32)
        return chosen, jnp.max(chosen, axis=1, keepdims=True)

    def prepare():
        acc[...] = jnp.zeros_like(acc)
        own[3].wait()

        @pl.loop(0, nz)
        def _(zz):
            start = pl.ds(pl.multiple_of(zz * width, width), width)
            chosen, taken = hits(zz * width, width)
            rhs_out[start, hd:] = chosen.astype(jnp.bfloat16)
            keep[start, :] = jnp.broadcast_to(1.0 - taken, (width, hd)).astype(jnp.bfloat16)

        lhs_out[:, :hd] = qb[0].reshape(group * tok, hd)

    def k_copy(i, source, target, rows, to):
        return remote(kb.at[source, 0, rows], kb.at[target, 0, rows], ksend.at[i], krecv.at[i], to)

    def b_copy(i, dz, rows, to):
        ref = bb.at[lax.rem(z + dz + nz, nz), xc, rows]
        return remote(ref, ref, bsend.at[i], brecv.at[i], to)

    rows_k, rows_b = pl.ds(0, BLK), pl.ds(0, held)
    key_z = {d: k_copy(d, 0, d, rows_k, dev(z + d, x, c)) for d in direct}
    bank_z = {d: b_copy(d, 0, rows_b, dev(z + d, x, c)) for d in direct}
    relays = {}
    if nz == 8:
        up, down = (1, 2), (7, 6)
        for i, source, target, part, parts_of, to in (
            (3, 2, 3, 0, 1, up[0]), (5, 6, 5, 0, 1, down[0]),
            (4, 2, 4, 0, 2, up[1]), (8, 6, 4, 1, 2, down[1]),
        ):
            rk = pl.ds(part * BLK // parts_of, BLK // parts_of)
            rb_ = pl.ds(part * held // parts_of, held // parts_of)
            key_z[i] = k_copy(i, source, target, rk, dev(z + to, x, c))
            bank_z[i] = b_copy(i, -source if source < 4 else nz - source, rb_, dev(z + to, x, c))
            relays.setdefault(source, []).append(i)

    key_core = {d: remote(kb.at[d, 0], kb.at[d, 1], dsend.at[d], drecv.at[d], sibling) for d in range(nz)}
    lo, hi = pl.ds(0, HEAD_CUT), pl.ds(HEAD_CUT, group - HEAD_CUT)

    def q_copy(i, src_slot, dst_slot, heads, target):
        return remote(qb.at[src_slot, heads], qb.at[dst_slot, heads], qsend.at[i], qrecv.at[i], target)

    q_x = [
        q_copy(0, 0, 1, lo, east), q_copy(1, 0, 1, hi, east),
        q_copy(2, 0, 3, hi, west), q_copy(3, 0, 3, lo, west),
        q_copy(4, 1, 2, lo, east), q_copy(5, 3, 2, hi, west),
    ]
    first, last = pl.ds(0, half_z), pl.ds(half_z, half_z)

    def c_copy(i, column, rows, target):
        return remote(bb.at[rows, column], bb.at[rows, column], cs.at[i], cr.at[i], target)

    def column(dx):
        return lax.rem(x + dx, NX) * 2 + c

    west_of, east_of = column(NX - 1), column(1)
    bank_x = [
        c_copy(0, xc, first, east), c_copy(1, xc, last, east),
        c_copy(2, xc, last, west), c_copy(3, xc, first, west),
        c_copy(4, west_of, first, east), c_copy(5, east_of, last, west),
    ]
    bank_in = [
        c_copy(0, west_of, first, east), c_copy(1, west_of, last, east),
        c_copy(2, east_of, last, west), c_copy(3, east_of, first, west),
        c_copy(4, column(2), first, east), c_copy(5, column(2), last, west),
    ]

    def e_copy(dx):
        return remote(bb.at[:, column(dx)], bb.at[:, column(dx)], es.at[dx], er.at[dx], sibling)

    bank_core = [e_copy(dx) for dx in range(NX)]
    near = [0, 1, nz - 1, 2][:per]

    def start_all():
        own[0].wait()
        for d in direct:
            key_z[d].start()
        key_core[0].start()
        own[1].wait()
        q_x[0].start()
        q_x[3].start()
        own[4].wait()
        prepare()

    def second_part():
        q_x[0].wait_send()
        q_x[1].start()
        q_x[3].wait_send()
        q_x[2].start()

    def pass_key(d):
        key_z[d].wait_recv()
        if d == 4 and nz == 8:
            key_z[8].wait_recv()
        for i in relays.get(d, ()):
            key_z[i].start()
        key_core[d].start()

    def pass_bank(d):
        bank_z[d].wait_recv()
        for i in relays.get(d, ()):
            bank_z[i].start()

    def have_keys(offsets):
        for d in offsets:
            key_core[d].wait_recv()

    def bank_rows():
        for i in bank_z:
            if i not in relays:
                bank_z[i].wait_recv()
        for i in (0, 2, 1, 3):
            bank_x[i].start()
        bank_core[0].start()

    def bank_forward():
        bank_in[0].wait_recv()
        bank_x[4].start()
        bank_in[2].wait_recv()
        bank_x[5].start()

    def bank_cross():
        bank_in[1].wait_recv()
        bank_core[3].start()
        bank_in[3].wait_recv()
        bank_core[1].start()

    def before(pair, g, part):
        if (pair, g, part) == (0, 0, 0):
            start_all()
            second_part()
            for d in direct[:2]:
                pass_key(d)
            own[2].wait()
            for d in direct:
                bank_z[d].start()
            for d in direct[2:]:
                pass_key(d)
            q_x[0].wait_recv()
            q_x[4].start()
            have_keys(near)
            q_x[3].wait_recv()
        if (pair, g, part) == (0, 0, 1):
            q_x[2].wait_recv()
            q_x[5].start()
            for d in (3, 5) if nz == 8 else ():
                pass_key(d)
            for d in relays:
                pass_bank(d)
            q_x[1].wait_recv()
        if (pair, g, part) == (0, 1, 0):
            pass_key(4)
            have_keys([d for d in range(nz) if d not in near])
        if (pair, g, part) == (1, 0, 0):
            q_x[4].wait_recv()
        if (pair, g, part) == (1, 0, 1):
            q_x[5].wait_recv()
            bank_rows()

    lane = lax.broadcasted_iota(jnp.int32, (1, BLK), 1)

    def compute(pair, g, part):
        tiles = (1 - pair, 3 - pair)
        offsets = near if groups == 1 else [6 * g, 1 + 2 * g, 7 - 2 * g, 2 + 2 * g]
        members = [(d, rel) for d in offsets for rel in range(2)]
        keys = jnp.concatenate([kb[d].reshape(2 * BLK, hd) for d in offsets], axis=0)
        position = [(z * 2 * NX + lax.rem(x - t + NX, NX) * 2 + c) * tok + lane for t in tiles]
        first_in, any_in = [], []
        for d, rel in members:
            begin = ws[(lax.rem(z - d + nz, nz) * NX + x) * 2 + (c + rel) % 2]
            hit = [(p >= begin) & (p < begin + WIN) for p in position]
            first_in.append(hit[0])
            any_in.append((hit[0] | hit[1]).astype(jnp.float32))
        sums = [acc[d, rel] for d, rel in members]
        for h in range(group)[HEAD_CUT:] if part else range(HEAD_CUT):
            rows = jnp.concatenate([qb[t, h] for t in tiles], axis=0)
            scores = lax.dot_general(
                keys, rows, (((1,), (1,)), ((), ())), preferred_element_type=jnp.float32
            )
            for i in range(len(members)):
                both = scores[i * BLK : (i + 1) * BLK]
                part_scores = jnp.where(first_in[i], both[:, :tok], both[:, tok:])
                top = jnp.max(part_scores, axis=0, keepdims=True)
                e = jnp.exp2((part_scores - top) * exp_scale)
                sums[i] = sums[i] + e * (any_in[i] / jnp.sum(e, axis=0, keepdims=True))
        for (d, rel), value in zip(members, sums):
            acc[d, rel] = value

    units = [(0, g, part) for g in range(groups) for part in range(2)]
    units += [(1, g, part) for part in range(2) for g in range(groups)]

    @pl.loop(0, len(units))
    def _(step):
        for k, unit in enumerate(units):
            pl.when(step == k)(functools.partial(before, *unit))
        pair = step // (2 * groups)
        rest = lax.rem(step, 2 * groups)
        g = jnp.where(pair == 0, rest // 2, lax.rem(rest, groups))
        part = jnp.where(pair == 0, lax.rem(rest, 2), rest // groups)
        for p in range(2):
            pl.when(part == p)(functools.partial(compute, pair, g, p))

    for d in range(nz):
        for rel in range(2):
            weight = jnp.sum(acc[d, rel], axis=1, keepdims=True)
            row = jnp.sum(weight * kb[d, rel].astype(jnp.float32), axis=0, keepdims=True)
            pb[(c + rel) % 2, pl.ds(lax.rem(z - d + nz, nz), 1), :] = row

    column_peers = [(dz, dc) for dz in range(nz) for dc in range(2) if dz or dc]
    parts = [
        remote(pb.at[(c + dc) % 2], rb.at[dz * 2 + dc], ps.at[dz * 2 + dc], pr.at[dz * 2 + dc], dev(z + dz, x, (c + dc) % 2))
        for dz, dc in column_peers
    ]
    for copy in parts:
        copy.start()
    rb[0] = pb[c]
    bank_forward()
    bank_cross()
    for copy in parts:
        copy.wait_recv()
    total = jnp.zeros((nz, hd), jnp.float32)
    for dz in range(nz):
        for dc in range(2):
            total = total + rb[lax.rem(z - dz + nz, nz) * 2 + (c + dc) % 2]
    mine = pl.ds(pl.multiple_of(xc * nz, nz), nz)
    rx[mine, :] = total / (group * WIN)
    row_peers = [(dx, dc) for dx in range(NX) for dc in range(2) if dx or dc]
    sums_x = [
        remote(rx.at[mine], rx.at[mine], xs.at[dx * 2 + dc], xr.at[dx * 2 + dc], dev(z, x + dx, (c + dc) % 2))
        for dx, dc in row_peers
    ]
    for copy in sums_x:
        copy.start()
    bank_in[4].wait_recv()
    bank_in[5].wait_recv()
    bank_core[2].start()
    for copy in [*key_z.values(), *key_core.values(), q_x[1], q_x[2], q_x[4], q_x[5], *bank_z.values(), *bank_x, *parts]:
        copy.wait_send()
    for copy in bank_core:
        copy.wait()

    @pl.loop(0, nz)
    def _(zz):
        start = pl.ds(pl.multiple_of(zz * width, width), width)
        rhs_out[start, :hd] = bb[zz].reshape(width, hd) * keep[start, :]

    chosen, taken = hits(s * held, held)
    for copy in sums_x:
        copy.wait_recv()
    ordered = [rx[pl.ds(zz, 2 * NX, stride=nz), :] for zz in range(nz)]
    reps = jnp.concatenate(ordered, axis=0).astype(jnp.bfloat16)
    value = lax.dot_general(
        lhs_out[:, :hd], jnp.concatenate([reps, reps], axis=0), (((1,), (1,)), ((), ())),
        preferred_element_type=jnp.float32,
    )
    high = value.astype(jnp.bfloat16).astype(jnp.float32)
    left = lax.broadcasted_iota(jnp.int32, (1, 2 * reps.shape[0]), 1) < reps.shape[0]
    lhs_out[:, hd:] = jnp.where(left, high, value - high).astype(jnp.bfloat16)
    placed = jnp.dot(
        chosen[:, : reps.shape[0]].astype(jnp.bfloat16), reps, preferred_element_type=jnp.float32
    )
    shard_out[...] = jnp.where(taken > 0.5, placed, bb[z, xc].astype(jnp.float32)).astype(jnp.bfloat16)
    for copy in sums_x:
        copy.wait_send()


def refresh(nz, window_start, slots, q, k, b):
    group, tok, hd = q.shape
    hbm = pl.BlockSpec(memory_space=pl.ANY)
    vmem = pl.BlockSpec(memory_space=VMEM)
    dma = pltpu.SemaphoreType.DMA
    bank_shape = (nz, 2 * NX, *b.shape)
    return pl.pallas_call(
        functools.partial(refresh_kernel, nz),
        out_shape=(
            on_chip((nz * 2 * NX * b.shape[0], hd + 2 * slots.shape[1]), jnp.bfloat16),
            on_chip((group * tok, hd + 2 * slots.shape[1]), jnp.bfloat16),
            on_chip(b.shape, jnp.bfloat16),
        ),
        in_specs=[hbm] * 5,
        out_specs=(vmem, vmem, vmem),
        scratch_shapes=[
            pltpu.SMEM(window_start.shape, jnp.int32),
            VMEM(slots.shape, jnp.int32),
            VMEM((NX, group, tok, hd), jnp.bfloat16),
            VMEM((nz, 2, BLK, hd), jnp.bfloat16),
            VMEM(bank_shape, jnp.bfloat16),
            VMEM((nz * 2 * NX * b.shape[0], hd), jnp.bfloat16),
            VMEM((nz, 2, BLK, BLK), jnp.float32),
            VMEM((2, nz, hd), jnp.float32),
            VMEM((2 * nz, nz, hd), jnp.float32),
            VMEM((2 * NX * nz, hd), jnp.float32),
            dma((5,)),
            dma((nz + 1,)), dma((nz + 1,)), dma((nz,)), dma((nz,)),
            dma((6,)), dma((6,)),
            dma((nz + 1,)), dma((nz + 1,)),
            dma((6,)), dma((6,)), dma((NX,)), dma((NX,)),
            dma((2 * nz,)), dma((2 * nz,)), dma((2 * NX,)), dma((2 * NX,)),
        ],
        compiler_params=pltpu.CompilerParams(collective_id=0, has_side_effects=True),
        name="refresh",
    )(window_start, slots, q, k, b)


def relevance_kernel(tile, lhs, rhs, shard, out, shard_out, held, sem):
    scale = 1.0 / math.sqrt(BLK)
    copies = [pltpu.make_async_copy(shard, shard_out, sem.at[0])]
    copies[0].start()
    for i in range(out.shape[1] // tile):
        cut = pl.ds(i * tile, tile)
        scores = lax.dot_general(
            lhs[...], rhs[cut, :], (((1,), (1,)), ((), ())), preferred_element_type=jnp.float32
        )
        held[:, cut] = (scores * scale).astype(jnp.bfloat16)
        copy = pltpu.make_async_copy(held.at[:, cut], out.at[:, cut], sem.at[i + 1])
        copy.start()
        copies.append(copy)
    for copy in copies:
        copy.wait()


def relevance_of(lhs, rhs, shard, tile=512):
    rows, total = lhs.shape[0], rhs.shape[0]
    vmem = pl.BlockSpec(memory_space=VMEM)
    hbm = pl.BlockSpec(memory_space=pl.ANY)
    lhs, rhs, shard = (kept(a) for a in (lhs, rhs, shard))
    return pl.pallas_call(
        functools.partial(relevance_kernel, tile),
        out_shape=(
            jax.ShapeDtypeStruct((rows, total), jnp.bfloat16),
            jax.ShapeDtypeStruct(shard.shape, jnp.bfloat16),
        ),
        in_specs=[vmem, vmem, vmem],
        out_specs=(hbm, hbm),
        scratch_shapes=[
            VMEM((rows, total), jnp.bfloat16),
            pltpu.SemaphoreType.DMA((1 + total // tile,)),
        ],
        name="relevance",
    )(lhs, rhs, shard)


def per_device(nz, queries, new_keys, cache_keys, window_start, owner_slot):
    tok, group, hd = queries.shape
    q = queries.transpose(1, 0, 2)
    rhs, lhs, shard = refresh(
        nz, window_start, owner_slot.reshape(1, -1), q, new_keys[:, 0, :], cache_keys[:, 0, :]
    )
    relevance, new_shard = relevance_of(lhs, rhs, shard)
    relevance = relevance.reshape(group, tok, rhs.shape[0]).transpose(1, 0, 2)
    return (relevance, new_shard[:, None, :])


def solution(mesh):
    nz = mesh.shape["seq"] // (2 * NX)
    split = P("seq", "kvh", None)
    return jax.shard_map(
        functools.partial(per_device, nz),
        mesh=mesh,
        in_specs=(split, split, split, P(), P()),
        out_specs=(split, split),
        check_vma=False,
    )
```

```python
import functools
import math

import jax
import jax.numpy as jnp
from jax import lax
from jax.experimental import pallas as pl
from jax.experimental.pallas import tpu as pltpu
from jax.sharding import PartitionSpec as P

BLK = 128
WIN = 512
NX = 4
HEAD_CUT = 4
MESH = pl.DeviceIdType.MESH
VMEM = pltpu.VMEM


def on_chip(shape, dtype):
    return VMEM(shape, dtype)


def kept(array):
    return pltpu.with_memory_space_constraint(array, VMEM)


def refresh_kernel(
    nz, ws_hbm, slots_hbm, q_hbm, k_hbm, b_hbm, rhs_out, lhs_out, shard_out,
    ws, slots, qb, kb, bb, keep, acc, pb, rb, rx,
    lsem, sent, come, krecv, drecv, qsend, qrecv, brecv, cr,
):
    group, tok, hd = q_hbm.shape
    held = b_hbm.shape[0]
    half_z = nz // 2
    per = min(4, nz)
    groups = nz // per
    s = lax.axis_index("seq")
    z, x, c = s // (2 * NX), (s // 2) % NX, s % 2
    xc = x * 2 + c
    exp_scale = math.log2(math.e) / math.sqrt(hd)

    def dev(zz, xx, cc):
        return {"seq": (lax.rem(zz, nz) * NX + lax.rem(xx, NX)) * 2 + cc}

    def remote(src, dst, ssem, rsem, target):
        return pltpu.make_async_remote_copy(
            src_ref=src, dst_ref=dst, send_sem=ssem, recv_sem=rsem,
            device_id=target, device_id_type=MESH,
        )

    sibling = dev(z, x, 1 - c)
    east, west = dev(z, x + 1, c), dev(z, x + NX - 1, c)

    own = [
        pltpu.make_async_copy(k_hbm, kb.at[0, 0], lsem.at[0]),
        pltpu.make_async_copy(q_hbm, qb.at[0], lsem.at[1]),
        pltpu.make_async_copy(b_hbm, bb.at[z, xc], lsem.at[2]),
        pltpu.make_async_copy(slots_hbm, slots, lsem.at[3]),
        pltpu.make_async_copy(ws_hbm, ws, lsem.at[4]),
    ]
    for copy in own:
        copy.start()

    direct = sorted({d % nz for d in (1, -1, 2, -2)} - {0}, key=lambda d: (min(d, nz - d), d))
    peers = [sibling, east, west] + [dev(z + d, x, c) for d in direct]
    barrier = pltpu.get_barrier_semaphore()
    for peer in peers:
        pl.semaphore_signal(barrier, inc=1, device_id=peer, device_id_type=MESH)

    pl.semaphore_wait(barrier, len(peers))

    width = 2 * NX * held

    def hits(first_row, count):
        columns = jnp.concatenate([slots[...], slots[...]], axis=1)
        row = first_row + lax.broadcasted_iota(jnp.int32, (count, columns.shape[1]), 0)
        chosen = (row == columns).astype(jnp.float32)
        return chosen, jnp.max(chosen, axis=1, keepdims=True)

    def prepare():
        acc[...] = jnp.zeros_like(acc)
        own[3].wait()

        @pl.loop(0, nz)
        def _(zz):
            start = pl.ds(pl.multiple_of(zz * width, width), width)
            chosen, taken = hits(zz * width, width)
            rhs_out[start, hd:] = chosen.astype(jnp.bfloat16)
            keep[start, :] = jnp.broadcast_to(1.0 - taken, (width, hd)).astype(jnp.bfloat16)

        lhs_out[:, :hd] = qb[0].reshape(group * tok, hd)

    def k_copy(i, source, target, rows, to):
        return remote(kb.at[source, 0, rows], kb.at[target, 0, rows], sent.at[0], krecv.at[i], to)

    def b_copy(i, dz, rows, to):
        ref = bb.at[lax.rem(z + dz + nz, nz), xc, rows]
        return remote(ref, ref, sent.at[1], brecv.at[i], to)

    rows_k, rows_b = pl.ds(0, BLK), pl.ds(0, held)
    key_z = {d: k_copy(d, 0, d, rows_k, dev(z + d, x, c)) for d in direct}
    bank_z = {d: b_copy(d, 0, rows_b, dev(z + d, x, c)) for d in direct}
    relays = {}
    if nz == 8:
        up, down = (1, 2), (7, 6)
        for i, source, target, part, parts_of, to in (
            (3, 2, 3, 0, 1, up[0]), (5, 6, 5, 0, 1, down[0]),
            (4, 2, 4, 0, 2, up[1]), (8, 6, 4, 1, 2, down[1]),
        ):
            rk = pl.ds(part * BLK // parts_of, BLK // parts_of)
            rb_ = pl.ds(part * held // parts_of, held // parts_of)
            key_z[i] = k_copy(i, source, target, rk, dev(z + to, x, c))
            bank_z[i] = b_copy(i, -source if source < 4 else nz - source, rb_, dev(z + to, x, c))
            relays.setdefault(source, []).append(i)

    key_core = {d: remote(kb.at[d, 0], kb.at[d, 1], sent.at[2], drecv.at[d], sibling) for d in range(nz)}
    lo, hi = pl.ds(0, HEAD_CUT), pl.ds(HEAD_CUT, group - HEAD_CUT)

    def q_copy(i, src_slot, dst_slot, heads, target):
        return remote(qb.at[src_slot, heads], qb.at[dst_slot, heads], qsend.at[i], qrecv.at[i], target)

    q_x = [
        q_copy(0, 0, 1, lo, east), q_copy(1, 0, 1, hi, east),
        q_copy(2, 0, 3, hi, west), q_copy(3, 0, 3, lo, west),
        q_copy(4, 1, 2, lo, east), q_copy(5, 3, 2, hi, west),
    ]
    first, last = pl.ds(0, half_z), pl.ds(half_z, half_z)

    def c_copy(i, column, rows, target):
        return remote(bb.at[rows, column], bb.at[rows, column], sent.at[3], cr.at[i], target)

    def column(dx):
        return lax.rem(x + dx, NX) * 2 + c

    west_of, east_of = column(NX - 1), column(1)
    bank_x = [
        c_copy(0, xc, first, east), c_copy(1, xc, last, east),
        c_copy(2, xc, last, west), c_copy(3, xc, first, west),
        c_copy(4, west_of, first, east), c_copy(5, east_of, last, west),
    ]
    bank_in = [
        c_copy(0, west_of, first, east), c_copy(1, west_of, last, east),
        c_copy(2, east_of, last, west), c_copy(3, east_of, first, west),
        c_copy(4, column(2), first, east), c_copy(5, column(2), last, west),
    ]

    def e_copy(dx):
        return remote(bb.at[:, column(dx)], bb.at[:, column(dx)], sent.at[4], come.at[0], sibling)

    bank_core = [e_copy(dx) for dx in range(NX)]
    near = [0, 1, nz - 1, 2][:per]

    def start_all():
        own[0].wait()
        for d in direct:
            key_z[d].start()
        key_core[0].start()
        own[1].wait()
        q_x[0].start()
        q_x[3].start()
        own[4].wait()
        prepare()

    def second_part():
        q_x[0].wait_send()
        q_x[1].start()
        q_x[3].wait_send()
        q_x[2].start()

    def pass_key(d):
        key_z[d].wait_recv()
        if d == 4 and nz == 8:
            key_z[8].wait_recv()
        for i in relays.get(d, ()):
            key_z[i].start()
        key_core[d].start()

    def pass_bank(d):
        bank_z[d].wait_recv()
        for i in relays.get(d, ()):
            bank_z[i].start()

    def have_keys(offsets):
        for d in offsets:
            key_core[d].wait_recv()

    def bank_rows():
        for i in bank_z:
            if i not in relays:
                bank_z[i].wait_recv()
        for i in (0, 2, 1, 3):
            bank_x[i].start()
        bank_core[0].start()

    def bank_forward():
        bank_in[0].wait_recv()
        bank_x[4].start()
        bank_in[2].wait_recv()
        bank_x[5].start()

    def bank_cross():
        bank_in[1].wait_recv()
        bank_core[3].start()
        bank_in[3].wait_recv()
        bank_core[1].start()

    def before(pair, g, part=0):
        if (pair, g, part) == (0, 0, 0):
            start_all()
            second_part()
            for d in direct[:2]:
                pass_key(d)
            own[2].wait()
            for d in direct:
                bank_z[d].start()
            for d in direct[2:]:
                pass_key(d)
            q_x[0].wait_recv()
            q_x[4].start()
            have_keys(near)
            q_x[3].wait_recv()
        if (pair, g, part) == (0, 0, 1):
            q_x[2].wait_recv()
            q_x[5].start()
            for d in (3, 5) if nz == 8 else ():
                pass_key(d)
            for d in relays:
                pass_bank(d)
            q_x[1].wait_recv()
        if (pair, g) == (0, 1):
            pass_key(4)
            have_keys([d for d in range(nz) if d not in near])
        if (pair, g) == (1, 0):
            q_x[4].wait_recv()
            q_x[5].wait_recv()
            bank_rows()

    lane = lax.broadcasted_iota(jnp.int32, (1, BLK), 1)

    def compute(pair, g, heads):
        tiles = (1 - pair, 3 - pair)
        offsets = near if groups == 1 else [6 * g, 1 + 2 * g, 7 - 2 * g, 2 + 2 * g]
        members = [(d, rel) for d in offsets for rel in range(2)]
        keys = jnp.concatenate([kb[d].reshape(2 * BLK, hd) for d in offsets], axis=0)
        position = [(z * 2 * NX + lax.rem(x - t + NX, NX) * 2 + c) * tok + lane for t in tiles]
        first_in, any_in = [], []
        for d, rel in members:
            begin = ws[(lax.rem(z - d + nz, nz) * NX + x) * 2 + (c + rel) % 2]
            hit = [(p >= begin) & (p < begin + WIN) for p in position]
            first_in.append(hit[0])
            any_in.append((hit[0] | hit[1]).astype(jnp.float32))
        sums = [acc[d, rel] for d, rel in members]
        for h in heads:
            rows = jnp.concatenate([qb[t, h] for t in tiles], axis=0)
            scores = lax.dot_general(
                keys, rows, (((1,), (1,)), ((), ())), preferred_element_type=jnp.float32
            )
            for i in range(len(members)):
                both = scores[i * BLK : (i + 1) * BLK]
                part_scores = jnp.where(first_in[i], both[:, :tok], both[:, tok:])
                top = jnp.max(part_scores, axis=0, keepdims=True)
                e = jnp.exp2((part_scores - top) * exp_scale)
                sums[i] = sums[i] + e * (any_in[i] / jnp.sum(e, axis=0, keepdims=True))
        for (d, rel), value in zip(members, sums):
            acc[d, rel] = value

    before(0, 0, 0)
    compute(0, 0, range(HEAD_CUT))
    before(0, 0, 1)
    compute(0, 0, range(HEAD_CUT, group))

    @pl.loop(1, 2 * groups)
    def _(step):
        for k in range(1, 2 * groups):
            pl.when(step == k)(functools.partial(before, k // groups, k % groups))
        compute(step // groups, lax.rem(step, groups), range(group))

    for d in range(nz):
        for rel in range(2):
            weight = jnp.sum(acc[d, rel], axis=1, keepdims=True)
            row = jnp.sum(weight * kb[d, rel].astype(jnp.float32), axis=0, keepdims=True)
            pb[(c + rel) % 2, pl.ds(lax.rem(z - d + nz, nz), 1), :] = row

    column_peers = [(dz, dc) for dz in range(nz) for dc in range(2) if dz or dc]
    parts = [
        remote(pb.at[(c + dc) % 2], rb.at[dz * 2 + dc], sent.at[5], come.at[1], dev(z + dz, x, (c + dc) % 2))
        for dz, dc in column_peers
    ]
    for copy in parts:
        copy.start()
    rb[0] = pb[c]
    bank_forward()
    bank_cross()
    def together(ref, i, j=0):
        return remote(ref, ref, sent.at[i], come.at[j], sibling)

    all_keys = together(kb.at[pl.ds(0, nz - 1), 0], 0)
    all_shards = together(bb.at[pl.ds(0, nz - 1), 0], 1)
    all_key_core = together(kb.at[:, 0], 2)
    all_bank_x = together(bb.at[:, pl.ds(0, 3)], 3)
    all_bank_core = together(bb.at[:, pl.ds(0, NX)], 4, 0)
    all_parts = together(rb.at[pl.ds(1, 2 * nz - 1)], 5, 1)
    all_sums = together(rx.at[pl.ds(0, (2 * NX - 1) * nz)], 6, 2)
    all_parts.wait_recv()
    total = jnp.zeros((nz, hd), jnp.float32)
    for dz in range(nz):
        for dc in range(2):
            total = total + rb[lax.rem(z - dz + nz, nz) * 2 + (c + dc) % 2]
    mine = pl.ds(pl.multiple_of(xc * nz, nz), nz)
    rx[mine, :] = total / (group * WIN)
    row_peers = [(dx, dc) for dx in range(NX) for dc in range(2) if dx or dc]
    sums_x = [
        remote(rx.at[mine], rx.at[mine], sent.at[6], come.at[2], dev(z, x + dx, (c + dc) % 2))
        for dx, dc in row_peers
    ]
    for copy in sums_x:
        copy.start()
    bank_in[4].wait_recv()
    bank_in[5].wait_recv()
    bank_core[2].start()
    for copy in (all_keys, all_shards, all_key_core, all_bank_x, all_parts, q_x[1], q_x[2], q_x[4], q_x[5]):
        copy.wait_send()
    all_bank_core.wait()

    @pl.loop(0, nz)
    def _(zz):
        start = pl.ds(pl.multiple_of(zz * width, width), width)
        rhs_out[start, :hd] = bb[zz].reshape(width, hd) * keep[start, :]

    chosen, taken = hits(s * held, held)
    all_sums.wait_recv()
    ordered = [rx[pl.ds(zz, 2 * NX, stride=nz), :] for zz in range(nz)]
    reps = jnp.concatenate(ordered, axis=0).astype(jnp.bfloat16)
    value = lax.dot_general(
        lhs_out[:, :hd], jnp.concatenate([reps, reps], axis=0), (((1,), (1,)), ((), ())),
        preferred_element_type=jnp.float32,
    )
    high = value.astype(jnp.bfloat16).astype(jnp.float32)
    left = lax.broadcasted_iota(jnp.int32, (1, 2 * reps.shape[0]), 1) < reps.shape[0]
    lhs_out[:, hd:] = jnp.where(left, high, value - high).astype(jnp.bfloat16)
    placed = jnp.dot(
        chosen[:, : reps.shape[0]].astype(jnp.bfloat16), reps, preferred_element_type=jnp.float32
    )
    shard_out[...] = jnp.where(taken > 0.5, placed, bb[z, xc].astype(jnp.float32)).astype(jnp.bfloat16)
    all_sums.wait_send()


def refresh(nz, window_start, slots, q, k, b):
    group, tok, hd = q.shape
    hbm = pl.BlockSpec(memory_space=pl.ANY)
    vmem = pl.BlockSpec(memory_space=VMEM)
    dma = pltpu.SemaphoreType.DMA
    bank_shape = (nz, 2 * NX, *b.shape)
    return pl.pallas_call(
        functools.partial(refresh_kernel, nz),
        out_shape=(
            on_chip((nz * 2 * NX * b.shape[0], hd + 2 * slots.shape[1]), jnp.bfloat16),
            on_chip((group * tok, hd + 2 * slots.shape[1]), jnp.bfloat16),
            on_chip(b.shape, jnp.bfloat16),
        ),
        in_specs=[hbm] * 5,
        out_specs=(vmem, vmem, vmem),
        scratch_shapes=[
            pltpu.SMEM(window_start.shape, jnp.int32),
            VMEM(slots.shape, jnp.int32),
            VMEM((NX, group, tok, hd), jnp.bfloat16),
            VMEM((nz, 2, BLK, hd), jnp.bfloat16),
            VMEM(bank_shape, jnp.bfloat16),
            VMEM((nz * 2 * NX * b.shape[0], hd), jnp.bfloat16),
            VMEM((nz, 2, BLK, BLK), jnp.float32),
            VMEM((2, nz, hd), jnp.float32),
            VMEM((2 * nz, nz, hd), jnp.float32),
            VMEM((2 * NX * nz, hd), jnp.float32),
            dma((5,)), dma((7,)), dma((3,)),
            dma((nz + 1,)), dma((nz,)), dma((6,)), dma((6,)), dma((nz + 1,)), dma((6,)),
        ],
        compiler_params=pltpu.CompilerParams(collective_id=0, has_side_effects=True),
        name="refresh",
    )(window_start, slots, q, k, b)


def relevance_kernel(tile, lhs, rhs, shard, out, shard_out, held, sem):
    scale = 1.0 / math.sqrt(BLK)
    copies = [pltpu.make_async_copy(shard, shard_out, sem.at[0])]
    copies[0].start()
    for i in range(out.shape[1] // tile):
        cut = pl.ds(i * tile, tile)
        scores = lax.dot_general(
            lhs[...], rhs[cut, :], (((1,), (1,)), ((), ())), preferred_element_type=jnp.float32
        )
        held[:, cut] = (scores * scale).astype(jnp.bfloat16)
        copy = pltpu.make_async_copy(held.at[:, cut], out.at[:, cut], sem.at[i + 1])
        copy.start()
        copies.append(copy)
    for copy in copies:
        copy.wait()


def relevance_of(lhs, rhs, shard, tile=512):
    rows, total = lhs.shape[0], rhs.shape[0]
    vmem = pl.BlockSpec(memory_space=VMEM)
    hbm = pl.BlockSpec(memory_space=pl.ANY)
    lhs, rhs, shard = (kept(a) for a in (lhs, rhs, shard))
    return pl.pallas_call(
        functools.partial(relevance_kernel, tile),
        out_shape=(
            jax.ShapeDtypeStruct((rows, total), jnp.bfloat16),
            jax.ShapeDtypeStruct(shard.shape, jnp.bfloat16),
        ),
        in_specs=[vmem, vmem, vmem],
        out_specs=(hbm, hbm),
        scratch_shapes=[
            VMEM((rows, total), jnp.bfloat16),
            pltpu.SemaphoreType.DMA((1 + total // tile,)),
        ],
        name="relevance",
    )(lhs, rhs, shard)


def per_device(nz, queries, new_keys, cache_keys, window_start, owner_slot):
    tok, group, hd = queries.shape
    q = queries.transpose(1, 0, 2)
    rhs, lhs, shard = refresh(
        nz, window_start, owner_slot.reshape(1, -1), q, new_keys[:, 0, :], cache_keys[:, 0, :]
    )
    relevance, new_shard = relevance_of(lhs, rhs, shard)
    relevance = relevance.reshape(group, tok, rhs.shape[0]).transpose(1, 0, 2)
    return (relevance, new_shard[:, None, :])


def solution(mesh):
    nz = mesh.shape["seq"] // (2 * NX)
    split = P("seq", "kvh", None)
    return jax.shard_map(
        functools.partial(per_device, nz),
        mesh=mesh,
        in_specs=(split, split, split, P(), P()),
        out_specs=(split, split),
        check_vma=False,
    )
```

```python
import functools
import math

import jax
import jax.numpy as jnp
from jax import lax
from jax.experimental import pallas as pl
from jax.experimental.pallas import tpu as pltpu
from jax.sharding import PartitionSpec as P

BLK = 128
WIN = 512
NX = 4
HEAD_CUT = 4
MESH = pl.DeviceIdType.MESH
VMEM = pltpu.VMEM


def on_chip(shape, dtype):
    return VMEM(shape, dtype)


def kept(array):
    return pltpu.with_memory_space_constraint(array, VMEM)


def refresh_kernel(
    nz, ws_hbm, slots_hbm, q_hbm, k_hbm, b_hbm, rhs_out, lhs_out, shard_out,
    ws, slots, qb, kb, bb, keep, acc, pb, rb, rx,
    lsem, sent, come, krecv, qsend, qrecv, brecv, cr,
):
    group, tok, hd = q_hbm.shape
    held = b_hbm.shape[0]
    half_z = nz // 2
    per = min(4, nz)
    groups = nz // per
    s = lax.axis_index("seq")
    z, x, c = s // (2 * NX), (s // 2) % NX, s % 2
    xc = x * 2 + c
    exp_scale = math.log2(math.e) / math.sqrt(hd)

    def dev(zz, xx, cc):
        return {"seq": (lax.rem(zz, nz) * NX + lax.rem(xx, NX)) * 2 + cc}

    def remote(src, dst, ssem, rsem, target):
        return pltpu.make_async_remote_copy(
            src_ref=src, dst_ref=dst, send_sem=ssem, recv_sem=rsem,
            device_id=target, device_id_type=MESH,
        )

    sibling = dev(z, x, 1 - c)
    east, west = dev(z, x + 1, c), dev(z, x + NX - 1, c)

    own = [
        pltpu.make_async_copy(k_hbm, kb.at[0, 0], lsem.at[0]),
        pltpu.make_async_copy(q_hbm, qb.at[0], lsem.at[1]),
        pltpu.make_async_copy(b_hbm, bb.at[z, xc], lsem.at[2]),
        pltpu.make_async_copy(slots_hbm, slots, lsem.at[3]),
        pltpu.make_async_copy(ws_hbm, ws, lsem.at[4]),
    ]
    for copy in own:
        copy.start()

    direct = sorted({d % nz for d in (1, -1, 2, -2)} - {0}, key=lambda d: (min(d, nz - d), d))
    peers = [sibling, east, west] + [dev(z + d, x, c) for d in direct]
    barrier = pltpu.get_barrier_semaphore()
    for peer in peers:
        pl.semaphore_signal(barrier, inc=1, device_id=peer, device_id_type=MESH)

    pl.semaphore_wait(barrier, len(peers))

    width = 2 * NX * held

    def hits(first_row, count):
        columns = jnp.concatenate([slots[...], slots[...]], axis=1)
        row = first_row + lax.broadcasted_iota(jnp.int32, (count, columns.shape[1]), 0)
        chosen = (row == columns).astype(jnp.float32)
        return chosen, jnp.max(chosen, axis=1, keepdims=True)

    def prepare():
        acc[...] = jnp.zeros_like(acc)
        own[3].wait()

        @pl.loop(0, nz)
        def _(zz):
            start = pl.ds(pl.multiple_of(zz * width, width), width)
            chosen, taken = hits(zz * width, width)
            rhs_out[start, hd:] = chosen.astype(jnp.bfloat16)
            keep[start, :] = jnp.broadcast_to(1.0 - taken, (width, hd)).astype(jnp.bfloat16)

        lhs_out[:, :hd] = qb[0].reshape(group * tok, hd)

    def k_copy(i, source, target, rows, to):
        return remote(kb.at[source, 0, rows], kb.at[target, 0, rows], sent.at[0], krecv.at[i], to)

    def b_copy(i, dz, rows, to):
        ref = bb.at[lax.rem(z + dz + nz, nz), xc, rows]
        return remote(ref, ref, sent.at[1], come.at[5] if i not in (2, 6) else brecv.at[i // 6], to)

    rows_k, rows_b = pl.ds(0, BLK), pl.ds(0, held)
    key_z = {d: k_copy(d, 0, d, rows_k, dev(z + d, x, c)) for d in direct}
    bank_z = {d: b_copy(d, 0, rows_b, dev(z + d, x, c)) for d in direct}
    relays = {}
    if nz == 8:
        up, down = (1, 2), (7, 6)
        for i, source, target, part, parts_of, to in (
            (3, 2, 3, 0, 1, up[0]), (5, 6, 5, 0, 1, down[0]),
            (4, 2, 4, 0, 2, up[1]), (8, 6, 4, 1, 2, down[1]),
        ):
            rk = pl.ds(part * BLK // parts_of, BLK // parts_of)
            rb_ = pl.ds(part * held // parts_of, held // parts_of)
            key_z[i] = k_copy(i, source, target, rk, dev(z + to, x, c))
            bank_z[i] = b_copy(i, -source if source < 4 else nz - source, rb_, dev(z + to, x, c))
            relays.setdefault(source, []).append(i)

    near = [0, 1, nz - 1, 2][:per]
    key_core = {d: remote(kb.at[d, 0], kb.at[d, 1], sent.at[2], come.at[3 if d in near else 4], sibling) for d in range(nz)}
    lo, hi = pl.ds(0, HEAD_CUT), pl.ds(HEAD_CUT, group - HEAD_CUT)

    def q_copy(i, src_slot, dst_slot, heads, target):
        return remote(qb.at[src_slot, heads], qb.at[dst_slot, heads], qsend.at[i], qrecv.at[i], target)

    q_x = [
        q_copy(0, 0, 1, lo, east), q_copy(1, 0, 1, hi, east),
        q_copy(2, 0, 3, hi, west), q_copy(3, 0, 3, lo, west),
        q_copy(4, 1, 2, lo, east), q_copy(5, 3, 2, hi, west),
    ]
    first, last = pl.ds(0, half_z), pl.ds(half_z, half_z)

    def c_copy(i, column, rows, target):
        return remote(bb.at[rows, column], bb.at[rows, column], sent.at[3], cr.at[i], target)

    def column(dx):
        return lax.rem(x + dx, NX) * 2 + c

    west_of, east_of = column(NX - 1), column(1)
    bank_x = [
        c_copy(0, xc, first, east), c_copy(1, xc, last, east),
        c_copy(2, xc, last, west), c_copy(3, xc, first, west),
        c_copy(4, west_of, first, east), c_copy(5, east_of, last, west),
    ]
    bank_in = [
        c_copy(0, west_of, first, east), c_copy(1, west_of, last, east),
        c_copy(2, east_of, last, west), c_copy(3, east_of, first, west),
        c_copy(4, column(2), first, east), c_copy(5, column(2), last, west),
    ]

    def e_copy(dx):
        return remote(bb.at[:, column(dx)], bb.at[:, column(dx)], sent.at[4], come.at[0], sibling)

    bank_core = [e_copy(dx) for dx in range(NX)]

    def together(ref, i, j=0):
        return remote(ref, ref, sent.at[i], come.at[j], sibling)

    all_keys = together(kb.at[pl.ds(0, nz - 1), 0], 0)
    all_shards = together(bb.at[pl.ds(0, nz - 1), 0], 1)
    all_key_core = together(kb.at[:, 0], 2)
    all_bank_x = together(bb.at[:, pl.ds(0, 3)], 3)
    all_bank_core = together(bb.at[:, pl.ds(0, NX)], 4, 0)
    all_parts = together(rb.at[pl.ds(1, 2 * nz - 1)], 5, 1)
    all_sums = together(rx.at[pl.ds(0, (2 * NX - 1) * nz)], 6, 2)
    near_keys = together(kb.at[pl.ds(0, per), 1], 2, 3)
    far_keys = together(kb.at[pl.ds(0, nz - per), 1], 2, 4) if groups > 1 else None
    rest_shards = together(bb.at[pl.ds(0, nz - 1 - len([d for d in direct if d in (2, 6)])), 0], 1, 5)

    def start_all():
        own[0].wait()
        for d in direct:
            key_z[d].start()
        key_core[0].start()
        own[1].wait()
        q_x[0].start()
        q_x[3].start()
        own[4].wait()
        prepare()

    def second_part():
        q_x[0].wait_send()
        q_x[1].start()
        q_x[3].wait_send()
        q_x[2].start()

    def pass_key(d):
        key_z[d].wait_recv()
        if d == 4 and nz == 8:
            key_z[8].wait_recv()
        for i in relays.get(d, ()):
            key_z[i].start()
        key_core[d].start()

    def pass_bank(d):
        bank_z[d].wait_recv()
        for i in relays.get(d, ()):
            bank_z[i].start()

    def bank_rows():
        rest_shards.wait_recv()
        for i in (2, 6):
            if i in bank_z and i not in relays:
                bank_z[i].wait_recv()
        for i in (0, 2, 1, 3):
            bank_x[i].start()
        bank_core[0].start()

    def bank_forward():
        bank_in[0].wait_recv()
        bank_x[4].start()
        bank_in[2].wait_recv()
        bank_x[5].start()

    def bank_cross():
        bank_in[1].wait_recv()
        bank_core[3].start()
        bank_in[3].wait_recv()
        bank_core[1].start()

    def before(pair, g, part=0):
        if (pair, g, part) == (0, 0, 0):
            start_all()
            second_part()
            for d in direct[:2]:
                pass_key(d)
            for d in direct[2:]:
                pass_key(d)
            q_x[0].wait_recv()
            q_x[4].start()
            near_keys.wait_recv()
            own[2].wait()
            for d in direct:
                bank_z[d].start()
            q_x[3].wait_recv()
        if (pair, g, part) == (0, 0, 1):
            q_x[2].wait_recv()
            q_x[5].start()
            for d in (3, 5) if nz == 8 else ():
                pass_key(d)
            q_x[1].wait_recv()
            if nz == 8:
                pass_key(4)
        if (pair, g) == (0, 1):
            far_keys.wait_recv()
            for d in relays:
                pass_bank(d)
        if (pair, g) == (1, 0):
            q_x[4].wait_recv()
            q_x[5].wait_recv()
            if groups == 1:
                bank_rows()
        if groups > 1 and (pair, g) == (1, groups - 1):
            bank_rows()

    lane = lax.broadcasted_iota(jnp.int32, (1, BLK), 1)

    def compute(pair, g, heads):
        tiles = (1 - pair, 3 - pair)
        offsets = near if groups == 1 else [6 * g, 1 + 2 * g, 7 - 2 * g, 2 + 2 * g]
        members = [(d, rel) for d in offsets for rel in range(2)]
        keys = jnp.concatenate([kb[d].reshape(2 * BLK, hd) for d in offsets], axis=0)
        position = [(z * 2 * NX + lax.rem(x - t + NX, NX) * 2 + c) * tok + lane for t in tiles]
        first_in, any_in = [], []
        for d, rel in members:
            begin = ws[(lax.rem(z - d + nz, nz) * NX + x) * 2 + (c + rel) % 2]
            hit = [(p >= begin) & (p < begin + WIN) for p in position]
            first_in.append(hit[0])
            any_in.append((hit[0] | hit[1]).astype(jnp.float32))
        sums = [acc[d, rel] for d, rel in members]
        for h in heads:
            rows = jnp.concatenate([qb[t, h] for t in tiles], axis=0)
            scores = lax.dot_general(
                keys, rows, (((1,), (1,)), ((), ())), preferred_element_type=jnp.float32
            )
            for i in range(len(members)):
                both = scores[i * BLK : (i + 1) * BLK]
                part_scores = jnp.where(first_in[i], both[:, :tok], both[:, tok:])
                top = jnp.max(part_scores, axis=0, keepdims=True)
                e = jnp.exp2((part_scores - top) * exp_scale)
                sums[i] = sums[i] + e * (any_in[i] / jnp.sum(e, axis=0, keepdims=True))
        for (d, rel), value in zip(members, sums):
            acc[d, rel] = value

    before(0, 0, 0)
    compute(0, 0, range(HEAD_CUT))
    before(0, 0, 1)
    compute(0, 0, range(HEAD_CUT, group))

    final = 2 * groups - 1

    @pl.loop(1, final)
    def _(step):
        for k in range(1, final):
            pl.when(step == k)(functools.partial(before, k // groups, k % groups))
        compute(step // groups, lax.rem(step, groups), range(group))

    def partial(offsets):
        for d in offsets:
            for rel in range(2):
                weight = jnp.sum(acc[d, rel], axis=1, keepdims=True)
                row = jnp.sum(weight * kb[d, rel].astype(jnp.float32), axis=0, keepdims=True)
                pb[(c + rel) % 2, pl.ds(lax.rem(z - d + nz, nz), 1), :] = row

    before(1, groups - 1)
    compute(1, groups - 1, range(group))
    if groups > 1:
        partial(near)
    partial([d for d in range(nz) if groups == 1 or d not in near])

    column_peers = [(dz, dc) for dz in range(nz) for dc in range(2) if dz or dc]
    column_peers.sort(key=lambda p: -min(p[0], nz - p[0]))
    parts = [
        remote(pb.at[(c + dc) % 2], rb.at[dz * 2 + dc], sent.at[5], come.at[1], dev(z + dz, x, (c + dc) % 2))
        for dz, dc in column_peers
    ]
    for copy in parts:
        copy.start()
    rb[0] = pb[c]
    bank_forward()
    bank_cross()
    all_parts.wait_recv()
    total = jnp.zeros((nz, hd), jnp.float32)
    for dz in range(nz):
        for dc in range(2):
            total = total + rb[lax.rem(z - dz + nz, nz) * 2 + (c + dc) % 2]
    mine = pl.ds(pl.multiple_of(xc * nz, nz), nz)
    rx[mine, :] = total / (group * WIN)
    row_peers = [(dx, dc) for dx in range(NX) for dc in range(2) if dx or dc]
    row_peers.sort(key=lambda p: -min(p[0], NX - p[0]))
    sums_x = [
        remote(rx.at[mine], rx.at[mine], sent.at[6], come.at[2], dev(z, x + dx, (c + dc) % 2))
        for dx, dc in row_peers
    ]
    for copy in sums_x:
        copy.start()
    bank_in[4].wait_recv()
    bank_in[5].wait_recv()
    bank_core[2].start()
    for copy in (all_keys, all_shards, all_key_core, all_bank_x, all_parts, q_x[1], q_x[2], q_x[4], q_x[5]):
        copy.wait_send()
    all_bank_core.wait()

    @pl.loop(0, nz)
    def _(zz):
        start = pl.ds(pl.multiple_of(zz * width, width), width)
        rhs_out[start, :hd] = bb[zz].reshape(width, hd) * keep[start, :]

    chosen, taken = hits(s * held, held)
    all_sums.wait_recv()
    ordered = [rx[pl.ds(zz, 2 * NX, stride=nz), :] for zz in range(nz)]
    reps = jnp.concatenate(ordered, axis=0).astype(jnp.bfloat16)
    value = lax.dot_general(
        lhs_out[:, :hd], jnp.concatenate([reps, reps], axis=0), (((1,), (1,)), ((), ())),
        preferred_element_type=jnp.float32,
    )
    high = value.astype(jnp.bfloat16).astype(jnp.float32)
    left = lax.broadcasted_iota(jnp.int32, (1, 2 * reps.shape[0]), 1) < reps.shape[0]
    lhs_out[:, hd:] = jnp.where(left, high, value - high).astype(jnp.bfloat16)
    placed = jnp.dot(
        chosen[:, : reps.shape[0]].astype(jnp.bfloat16), reps, preferred_element_type=jnp.float32
    )
    shard_out[...] = jnp.where(taken > 0.5, placed, bb[z, xc].astype(jnp.float32)).astype(jnp.bfloat16)
    all_sums.wait_send()


def refresh(nz, window_start, slots, q, k, b):
    group, tok, hd = q.shape
    hbm = pl.BlockSpec(memory_space=pl.ANY)
    vmem = pl.BlockSpec(memory_space=VMEM)
    dma = pltpu.SemaphoreType.DMA
    bank_shape = (nz, 2 * NX, *b.shape)
    return pl.pallas_call(
        functools.partial(refresh_kernel, nz),
        out_shape=(
            on_chip((nz * 2 * NX * b.shape[0], hd + 2 * slots.shape[1]), jnp.bfloat16),
            on_chip((group * tok, hd + 2 * slots.shape[1]), jnp.bfloat16),
            on_chip(b.shape, jnp.bfloat16),
        ),
        in_specs=[hbm] * 5,
        out_specs=(vmem, vmem, vmem),
        scratch_shapes=[
            pltpu.SMEM(window_start.shape, jnp.int32),
            VMEM(slots.shape, jnp.int32),
            VMEM((NX, group, tok, hd), jnp.bfloat16),
            VMEM((nz, 2, BLK, hd), jnp.bfloat16),
            VMEM(bank_shape, jnp.bfloat16),
            VMEM((nz * 2 * NX * b.shape[0], hd), jnp.bfloat16),
            VMEM((nz, 2, BLK, BLK), jnp.float32),
            VMEM((2, nz, hd), jnp.float32),
            VMEM((2 * nz, nz, hd), jnp.float32),
            VMEM((2 * NX * nz, hd), jnp.float32),
            dma((5,)), dma((7,)), dma((6,)),
            dma((nz + 1,)), dma((6,)), dma((6,)), dma((2,)), dma((6,)),
        ],
        compiler_params=pltpu.CompilerParams(collective_id=0, has_side_effects=True),
        name="refresh",
    )(window_start, slots, q, k, b)


def relevance_kernel(tile, lhs, rhs, shard, out, shard_out, held, sem):
    scale = 1.0 / math.sqrt(BLK)
    copies = [pltpu.make_async_copy(shard, shard_out, sem.at[0])]
    copies[0].start()
    for i in range(out.shape[1] // tile):
        cut = pl.ds(i * tile, tile)
        scores = lax.dot_general(
            lhs[...], rhs[cut, :], (((1,), (1,)), ((), ())), preferred_element_type=jnp.float32
        )
        held[:, cut] = (scores * scale).astype(jnp.bfloat16)
        copy = pltpu.make_async_copy(held.at[:, cut], out.at[:, cut], sem.at[i + 1])
        copy.start()
        copies.append(copy)
    for copy in copies:
        copy.wait()


def relevance_of(lhs, rhs, shard, tile=512):
    rows, total = lhs.shape[0], rhs.shape[0]
    vmem = pl.BlockSpec(memory_space=VMEM)
    hbm = pl.BlockSpec(memory_space=pl.ANY)
    lhs, rhs, shard = (kept(a) for a in (lhs, rhs, shard))
    return pl.pallas_call(
        functools.partial(relevance_kernel, tile),
        out_shape=(
            jax.ShapeDtypeStruct((rows, total), jnp.bfloat16),
            jax.ShapeDtypeStruct(shard.shape, jnp.bfloat16),
        ),
        in_specs=[vmem, vmem, vmem],
        out_specs=(hbm, hbm),
        scratch_shapes=[
            VMEM((rows, total), jnp.bfloat16),
            pltpu.SemaphoreType.DMA((1 + total // tile,)),
        ],
        name="relevance",
    )(lhs, rhs, shard)


def per_device(nz, queries, new_keys, cache_keys, window_start, owner_slot):
    tok, group, hd = queries.shape
    q = queries.transpose(1, 0, 2)
    rhs, lhs, shard = refresh(
        nz, window_start, owner_slot.reshape(1, -1), q, new_keys[:, 0, :], cache_keys[:, 0, :]
    )
    relevance, new_shard = relevance_of(lhs, rhs, shard)
    relevance = relevance.reshape(group, tok, rhs.shape[0]).transpose(1, 0, 2)
    return (relevance, new_shard[:, None, :])


def solution(mesh):
    nz = mesh.shape["seq"] // (2 * NX)
    split = P("seq", "kvh", None)
    return jax.shard_map(
        functools.partial(per_device, nz),
        mesh=mesh,
        in_specs=(split, split, split, P(), P()),
        out_specs=(split, split),
        check_vma=False,
    )
```

```python
import functools
import math

import jax
import jax.numpy as jnp
from jax import lax
from jax.experimental import pallas as pl
from jax.experimental.pallas import tpu as pltpu
from jax.sharding import PartitionSpec as P

BLK = 128
WIN = 512
NX = 4
HEAD_CUT = 4
MESH = pl.DeviceIdType.MESH
VMEM = pltpu.VMEM


def on_chip(shape, dtype):
    return VMEM(shape, dtype)


def kept(array):
    return pltpu.with_memory_space_constraint(array, VMEM)


def refresh_kernel(
    nz, ws_hbm, slots_hbm, q_hbm, k_hbm, b_hbm, rhs_out, lhs_out, shard_out,
    ws, slots, qb, kb, bb, keep, acc, pb, rb, rx,
    lsem, sent, come, krecv, qsend, qrecv, cr,
):
    group, tok, hd = q_hbm.shape
    held = b_hbm.shape[0]
    half_z = nz // 2
    per = min(4, nz)
    groups = nz // per
    s = lax.axis_index("seq")
    z, x, c = s // (2 * NX), (s // 2) % NX, s % 2
    xc = x * 2 + c
    exp_scale = math.log2(math.e) / math.sqrt(hd)

    def dev(zz, xx, cc):
        return {"seq": (lax.rem(zz, nz) * NX + lax.rem(xx, NX)) * 2 + cc}

    def remote(src, dst, ssem, rsem, target):
        return pltpu.make_async_remote_copy(
            src_ref=src, dst_ref=dst, send_sem=ssem, recv_sem=rsem,
            device_id=target, device_id_type=MESH,
        )

    sibling = dev(z, x, 1 - c)
    east, west = dev(z, x + 1, c), dev(z, x + NX - 1, c)

    own = [
        pltpu.make_async_copy(k_hbm, kb.at[0, 0], lsem.at[0]),
        pltpu.make_async_copy(q_hbm, qb.at[0], lsem.at[1]),
        pltpu.make_async_copy(b_hbm, bb.at[z, xc], lsem.at[2]),
        pltpu.make_async_copy(slots_hbm, slots, lsem.at[3]),
        pltpu.make_async_copy(ws_hbm, ws, lsem.at[4]),
    ]
    for copy in own:
        copy.start()

    direct = sorted({d % nz for d in (1, -1, 2, -2)} - {0}, key=lambda d: (min(d, nz - d), d))
    peers = [sibling, east, west] + [dev(z + d, x, c) for d in direct]
    barrier = pltpu.get_barrier_semaphore()
    for peer in peers:
        pl.semaphore_signal(barrier, inc=1, device_id=peer, device_id_type=MESH)

    pl.semaphore_wait(barrier, len(peers))

    width = 2 * NX * held

    def hits(first_row, count):
        columns = jnp.concatenate([slots[...], slots[...]], axis=1)
        row = first_row + lax.broadcasted_iota(jnp.int32, (count, columns.shape[1]), 0)
        chosen = (row == columns).astype(jnp.float32)
        return chosen, jnp.max(chosen, axis=1, keepdims=True)

    def prepare():
        acc[...] = jnp.zeros_like(acc)
        own[3].wait()

        @pl.loop(0, nz)
        def _(zz):
            start = pl.ds(pl.multiple_of(zz * width, width), width)
            chosen, taken = hits(zz * width, width)
            rhs_out[start, hd:] = chosen.astype(jnp.bfloat16)
            keep[start, :] = jnp.broadcast_to(1.0 - taken, (width, hd)).astype(jnp.bfloat16)

        lhs_out[:, :hd] = qb[0].reshape(group * tok, hd)

    def k_copy(i, source, target, rows, to):
        return remote(kb.at[source, 0, rows], kb.at[target, 0, rows], sent.at[0], krecv.at[i], to)

    def b_copy(i, dz, rows, to):
        ref = bb.at[lax.rem(z + dz + nz, nz), xc, rows]
        return remote(ref, ref, sent.at[1], come.at[5], to)

    rows_k, rows_b = pl.ds(0, BLK), pl.ds(0, held)
    key_z = {d: k_copy(d, 0, d, rows_k, dev(z + d, x, c)) for d in direct}
    bank_z = {d: b_copy(0, 0, rows_b, dev(z + d, x, c)) for d in range(1, nz)}
    relays = {}
    if nz == 8:
        up, down = (1, 2), (7, 6)
        for i, source, target, part, parts_of, to in (
            (3, 2, 3, 0, 1, up[0]), (5, 6, 5, 0, 1, down[0]),
            (4, 2, 4, 0, 2, up[1]), (8, 6, 4, 1, 2, down[1]),
        ):
            rk = pl.ds(part * BLK // parts_of, BLK // parts_of)
            key_z[i] = k_copy(i, source, target, rk, dev(z + to, x, c))
            relays.setdefault(source, []).append(i)

    near = [0, 1, nz - 1, 2][:per]
    key_core = {d: remote(kb.at[d, 0], kb.at[d, 1], sent.at[2], come.at[3 if d in near else 4], sibling) for d in range(nz)}
    lo, hi = pl.ds(0, HEAD_CUT), pl.ds(HEAD_CUT, group - HEAD_CUT)

    def q_copy(i, src_slot, dst_slot, heads, target):
        return remote(qb.at[src_slot, heads], qb.at[dst_slot, heads], qsend.at[i], qrecv.at[i], target)

    q_x = [
        q_copy(0, 0, 1, lo, east), q_copy(1, 0, 1, hi, east),
        q_copy(2, 0, 3, hi, west), q_copy(3, 0, 3, lo, west),
        q_copy(4, 1, 2, lo, east), q_copy(5, 3, 2, hi, west),
    ]
    first, last = pl.ds(0, half_z), pl.ds(half_z, half_z)

    def c_copy(i, column, rows, target):
        return remote(bb.at[rows, column], bb.at[rows, column], sent.at[3], cr.at[i], target)

    def column(dx):
        return lax.rem(x + dx, NX) * 2 + c

    west_of, east_of = column(NX - 1), column(1)
    bank_x = [
        c_copy(0, xc, first, east), c_copy(1, xc, last, east),
        c_copy(2, xc, last, west), c_copy(3, xc, first, west),
        c_copy(4, west_of, first, east), c_copy(5, east_of, last, west),
    ]
    bank_in = [
        c_copy(0, west_of, first, east), c_copy(1, west_of, last, east),
        c_copy(2, east_of, last, west), c_copy(3, east_of, first, west),
        c_copy(4, column(2), first, east), c_copy(5, column(2), last, west),
    ]

    def e_copy(dx):
        return remote(bb.at[:, column(dx)], bb.at[:, column(dx)], sent.at[4], come.at[0], sibling)

    bank_core = [e_copy(dx) for dx in range(NX)]

    def together(ref, i, j=0):
        return remote(ref, ref, sent.at[i], come.at[j], sibling)

    all_keys = together(kb.at[pl.ds(0, nz - 1), 0], 0)
    all_shards = together(bb.at[pl.ds(0, nz - 1), 0], 1)
    all_key_core = together(kb.at[:, 0], 2)
    all_bank_x = together(bb.at[:, pl.ds(0, 3)], 3)
    all_bank_core = together(bb.at[:, pl.ds(0, NX)], 4, 0)
    all_parts = together(rb.at[pl.ds(1, 2 * nz - 1)], 5, 1)
    all_sums = together(rx.at[pl.ds(0, (2 * NX - 1) * nz)], 6, 2)
    near_keys = together(kb.at[pl.ds(0, per), 1], 2, 3)
    far_keys = together(kb.at[pl.ds(0, nz - per), 1], 2, 4) if groups > 1 else None
    rest_shards = together(bb.at[pl.ds(0, nz - 1), 0], 1, 5)

    def start_all():
        own[0].wait()
        for d in direct:
            key_z[d].start()
        key_core[0].start()
        own[1].wait()
        q_x[0].start()
        q_x[3].start()
        own[4].wait()
        prepare()

    def second_part():
        q_x[0].wait_send()
        q_x[1].start()
        q_x[3].wait_send()
        q_x[2].start()

    def pass_key(d):
        key_z[d].wait_recv()
        if d == 4 and nz == 8:
            key_z[8].wait_recv()
        for i in relays.get(d, ()):
            key_z[i].start()
        key_core[d].start()

    def bank_rows():
        rest_shards.wait_recv()
        for i in (0, 2, 1, 3):
            bank_x[i].start()
        bank_core[0].start()

    def bank_forward():
        bank_in[0].wait_recv()
        bank_x[4].start()
        bank_in[2].wait_recv()
        bank_x[5].start()

    def bank_cross():
        bank_in[1].wait_recv()
        bank_core[3].start()
        bank_in[3].wait_recv()
        bank_core[1].start()

    def before(pair, g, part=0):
        if (pair, g, part) == (0, 0, 0):
            start_all()
            second_part()
            for d in direct[:2]:
                pass_key(d)
            for d in direct[2:]:
                pass_key(d)
            q_x[0].wait_recv()
            q_x[4].start()
            near_keys.wait_recv()
            own[2].wait()
            for d in direct:
                bank_z[d].start()
            q_x[3].wait_recv()
        if (pair, g, part) == (0, 0, 1):
            q_x[2].wait_recv()
            q_x[5].start()
            for d in (3, 5, 4) if nz == 8 else ():
                pass_key(d)
            for d in range(1, nz):
                if d not in direct:
                    bank_z[d].start()
            q_x[1].wait_recv()
        if (pair, g) == (0, 1):
            far_keys.wait_recv()
        if (pair, g) == (1, 0):
            q_x[4].wait_recv()
            q_x[5].wait_recv()
            if groups == 1:
                bank_rows()
        if groups > 1 and (pair, g) == (1, groups - 1):
            bank_rows()

    lane = lax.broadcasted_iota(jnp.int32, (1, BLK), 1)

    def compute(pair, g, heads):
        tiles = (1 - pair, 3 - pair)
        offsets = near if groups == 1 else [6 * g, 1 + 2 * g, 7 - 2 * g, 2 + 2 * g]
        members = [(d, rel) for d in offsets for rel in range(2)]
        keys = jnp.concatenate([kb[d].reshape(2 * BLK, hd) for d in offsets], axis=0)
        position = [(z * 2 * NX + lax.rem(x - t + NX, NX) * 2 + c) * tok + lane for t in tiles]
        first_in, any_in = [], []
        for d, rel in members:
            begin = ws[(lax.rem(z - d + nz, nz) * NX + x) * 2 + (c + rel) % 2]
            hit = [(p >= begin) & (p < begin + WIN) for p in position]
            first_in.append(hit[0])
            any_in.append((hit[0] | hit[1]).astype(jnp.float32))
        sums = [acc[d, rel] for d, rel in members]
        for h in heads:
            rows = jnp.concatenate([qb[t, h] for t in tiles], axis=0)
            scores = lax.dot_general(
                keys, rows, (((1,), (1,)), ((), ())), preferred_element_type=jnp.float32
            )
            for i in range(len(members)):
                both = scores[i * BLK : (i + 1) * BLK]
                part_scores = jnp.where(first_in[i], both[:, :tok], both[:, tok:])
                top = jnp.max(part_scores, axis=0, keepdims=True)
                e = jnp.exp2((part_scores - top) * exp_scale)
                sums[i] = sums[i] + e * (any_in[i] / jnp.sum(e, axis=0, keepdims=True))
        for (d, rel), value in zip(members, sums):
            acc[d, rel] = value

    before(0, 0, 0)
    compute(0, 0, range(HEAD_CUT))
    before(0, 0, 1)
    compute(0, 0, range(HEAD_CUT, group))

    final = 2 * groups - 1

    @pl.loop(1, final)
    def _(step):
        for k in range(1, final):
            pl.when(step == k)(functools.partial(before, k // groups, k % groups))
        compute(step // groups, lax.rem(step, groups), range(group))

    def partial(offsets):
        for d in offsets:
            for rel in range(2):
                weight = jnp.sum(acc[d, rel], axis=1, keepdims=True)
                row = jnp.sum(weight * kb[d, rel].astype(jnp.float32), axis=0, keepdims=True)
                pb[(c + rel) % 2, pl.ds(lax.rem(z - d + nz, nz), 1), :] = row

    before(1, groups - 1)
    compute(1, groups - 1, range(group))
    if groups > 1:
        partial(near)
    partial([d for d in range(nz) if groups == 1 or d not in near])

    column_peers = [(dz, dc) for dz in range(nz) for dc in range(2) if dz or dc]
    column_peers.sort(key=lambda p: -min(p[0], nz - p[0]))
    parts = [
        remote(pb.at[(c + dc) % 2], rb.at[dz * 2 + dc], sent.at[5], come.at[1], dev(z + dz, x, (c + dc) % 2))
        for dz, dc in column_peers
    ]
    for copy in parts:
        copy.start()
    rb[0] = pb[c]
    bank_forward()
    bank_cross()
    all_parts.wait_recv()
    total = jnp.zeros((nz, hd), jnp.float32)
    for dz in range(nz):
        for dc in range(2):
            total = total + rb[lax.rem(z - dz + nz, nz) * 2 + (c + dc) % 2]
    mine = pl.ds(pl.multiple_of(xc * nz, nz), nz)
    rx[mine, :] = total / (group * WIN)
    row_peers = [(dx, dc) for dx in range(NX) for dc in range(2) if dx or dc]
    row_peers.sort(key=lambda p: -min(p[0], NX - p[0]))
    sums_x = [
        remote(rx.at[mine], rx.at[mine], sent.at[6], come.at[2], dev(z, x + dx, (c + dc) % 2))
        for dx, dc in row_peers
    ]
    for copy in sums_x:
        copy.start()
    bank_in[4].wait_recv()
    bank_in[5].wait_recv()
    bank_core[2].start()
    for copy in (all_keys, all_shards, all_key_core, all_bank_x, all_parts, q_x[1], q_x[2], q_x[4], q_x[5]):
        copy.wait_send()
    all_bank_core.wait()

    @pl.loop(0, nz)
    def _(zz):
        start = pl.ds(pl.multiple_of(zz * width, width), width)
        rhs_out[start, :hd] = bb[zz].reshape(width, hd) * keep[start, :]

    chosen, taken = hits(s * held, held)
    all_sums.wait_recv()
    ordered = [rx[pl.ds(zz, 2 * NX, stride=nz), :] for zz in range(nz)]
    reps = jnp.concatenate(ordered, axis=0).astype(jnp.bfloat16)
    value = lax.dot_general(
        lhs_out[:, :hd], jnp.concatenate([reps, reps], axis=0), (((1,), (1,)), ((), ())),
        preferred_element_type=jnp.float32,
    )
    high = value.astype(jnp.bfloat16).astype(jnp.float32)
    left = lax.broadcasted_iota(jnp.int32, (1, 2 * reps.shape[0]), 1) < reps.shape[0]
    lhs_out[:, hd:] = jnp.where(left, high, value - high).astype(jnp.bfloat16)
    placed = jnp.dot(
        chosen[:, : reps.shape[0]].astype(jnp.bfloat16), reps, preferred_element_type=jnp.float32
    )
    shard_out[...] = jnp.where(taken > 0.5, placed, bb[z, xc].astype(jnp.float32)).astype(jnp.bfloat16)
    all_sums.wait_send()


def refresh(nz, window_start, slots, q, k, b):
    group, tok, hd = q.shape
    hbm = pl.BlockSpec(memory_space=pl.ANY)
    vmem = pl.BlockSpec(memory_space=VMEM)
    dma = pltpu.SemaphoreType.DMA
    bank_shape = (nz, 2 * NX, *b.shape)
    return pl.pallas_call(
        functools.partial(refresh_kernel, nz),
        out_shape=(
            on_chip((nz * 2 * NX * b.shape[0], hd + 2 * slots.shape[1]), jnp.bfloat16),
            on_chip((group * tok, hd + 2 * slots.shape[1]), jnp.bfloat16),
            on_chip(b.shape, jnp.bfloat16),
        ),
        in_specs=[hbm] * 5,
        out_specs=(vmem, vmem, vmem),
        scratch_shapes=[
            pltpu.SMEM(window_start.shape, jnp.int32),
            VMEM(slots.shape, jnp.int32),
            VMEM((NX, group, tok, hd), jnp.bfloat16),
            VMEM((nz, 2, BLK, hd), jnp.bfloat16),
            VMEM(bank_shape, jnp.bfloat16),
            VMEM((nz * 2 * NX * b.shape[0], hd), jnp.bfloat16),
            VMEM((nz, 2, BLK, BLK), jnp.float32),
            VMEM((2, nz, hd), jnp.float32),
            VMEM((2 * nz, nz, hd), jnp.float32),
            VMEM((2 * NX * nz, hd), jnp.float32),
            dma((5,)), dma((7,)), dma((6,)),
            dma((nz + 1,)), dma((6,)), dma((6,)), dma((6,)),
        ],
        compiler_params=pltpu.CompilerParams(collective_id=0, has_side_effects=True),
        name="refresh",
    )(window_start, slots, q, k, b)


def relevance_kernel(tile, lhs, rhs, shard, out, shard_out, held, sem):
    scale = 1.0 / math.sqrt(BLK)
    copies = [pltpu.make_async_copy(shard, shard_out, sem.at[0])]
    copies[0].start()
    for i in range(out.shape[1] // tile):
        cut = pl.ds(i * tile, tile)
        scores = lax.dot_general(
            lhs[...], rhs[cut, :], (((1,), (1,)), ((), ())), preferred_element_type=jnp.float32
        )
        held[:, cut] = (scores * scale).astype(jnp.bfloat16)
        copy = pltpu.make_async_copy(held.at[:, cut], out.at[:, cut], sem.at[i + 1])
        copy.start()
        copies.append(copy)
    for copy in copies:
        copy.wait()


def relevance_of(lhs, rhs, shard, tile=512):
    rows, total = lhs.shape[0], rhs.shape[0]
    vmem = pl.BlockSpec(memory_space=VMEM)
    hbm = pl.BlockSpec(memory_space=pl.ANY)
    lhs, rhs, shard = (kept(a) for a in (lhs, rhs, shard))
    return pl.pallas_call(
        functools.partial(relevance_kernel, tile),
        out_shape=(
            jax.ShapeDtypeStruct((rows, total), jnp.bfloat16),
            jax.ShapeDtypeStruct(shard.shape, jnp.bfloat16),
        ),
        in_specs=[vmem, vmem, vmem],
        out_specs=(hbm, hbm),
        scratch_shapes=[
            VMEM((rows, total), jnp.bfloat16),
            pltpu.SemaphoreType.DMA((1 + total // tile,)),
        ],
        name="relevance",
    )(lhs, rhs, shard)


def per_device(nz, queries, new_keys, cache_keys, window_start, owner_slot):
    tok, group, hd = queries.shape
    q = queries.transpose(1, 0, 2)
    rhs, lhs, shard = refresh(
        nz, window_start, owner_slot.reshape(1, -1), q, new_keys[:, 0, :], cache_keys[:, 0, :]
    )
    relevance, new_shard = relevance_of(lhs, rhs, shard)
    relevance = relevance.reshape(group, tok, rhs.shape[0]).transpose(1, 0, 2)
    return (relevance, new_shard[:, None, :])


def solution(mesh):
    nz = mesh.shape["seq"] // (2 * NX)
    split = P("seq", "kvh", None)
    return jax.shard_map(
        functools.partial(per_device, nz),
        mesh=mesh,
        in_specs=(split, split, split, P(), P()),
        out_specs=(split, split),
        check_vma=False,
    )
```

```python
import functools
import math

import jax
import jax.numpy as jnp
from jax import lax
from jax.experimental import pallas as pl
from jax.experimental.pallas import tpu as pltpu
from jax.sharding import PartitionSpec as P

BLK = 128
WIN = 512
NX = 4
HEAD_CUT = 4
MESH = pl.DeviceIdType.MESH
VMEM = pltpu.VMEM


def on_chip(shape, dtype):
    return VMEM(shape, dtype)


def kept(array):
    return pltpu.with_memory_space_constraint(array, VMEM)


def refresh_kernel(
    nz, ws_hbm, slots_hbm, q_hbm, k_hbm, b_hbm, rhs_out, lhs_out, shard_out,
    ws, slots, qb, kb, bb, keep, acc, pb, rb, rx,
    lsem, sent, come, krecv, qsend, qrecv, cr,
):
    group, tok, hd = q_hbm.shape
    held = b_hbm.shape[0]
    half_z = nz // 2
    per = min(4, nz)
    groups = nz // per
    s = lax.axis_index("seq")
    z, x, c = s // (2 * NX), (s // 2) % NX, s % 2
    xc = x * 2 + c
    exp_scale = math.log2(math.e) / math.sqrt(hd)

    def dev(zz, xx, cc):
        return {"seq": (lax.rem(zz, nz) * NX + lax.rem(xx, NX)) * 2 + cc}

    def remote(src, dst, ssem, rsem, target):
        return pltpu.make_async_remote_copy(
            src_ref=src, dst_ref=dst, send_sem=ssem, recv_sem=rsem,
            device_id=target, device_id_type=MESH,
        )

    sibling = dev(z, x, 1 - c)
    east, west = dev(z, x + 1, c), dev(z, x + NX - 1, c)

    own = [
        pltpu.make_async_copy(k_hbm, kb.at[0, 0], lsem.at[0]),
        pltpu.make_async_copy(q_hbm, qb.at[0], lsem.at[1]),
        pltpu.make_async_copy(b_hbm, bb.at[z, xc], lsem.at[2]),
        pltpu.make_async_copy(slots_hbm, slots, lsem.at[3]),
        pltpu.make_async_copy(ws_hbm, ws, lsem.at[4]),
    ]
    for copy in own:
        copy.start()

    direct = sorted({d % nz for d in (1, -1, 2, -2)} - {0}, key=lambda d: (min(d, nz - d), d))
    peers = [sibling, east, west] + [dev(z + d, x, c) for d in direct]
    barrier = pltpu.get_barrier_semaphore()
    for peer in peers:
        pl.semaphore_signal(barrier, inc=1, device_id=peer, device_id_type=MESH)

    pl.semaphore_wait(barrier, len(peers))

    width = 2 * NX * held

    def hits(first_row, count):
        columns = jnp.concatenate([slots[...], slots[...]], axis=1)
        row = first_row + lax.broadcasted_iota(jnp.int32, (count, columns.shape[1]), 0)
        chosen = (row == columns).astype(jnp.float32)
        return chosen, jnp.max(chosen, axis=1, keepdims=True)

    def prepare():
        acc[...] = jnp.zeros_like(acc)
        own[3].wait()

        @pl.loop(0, nz)
        def _(zz):
            start = pl.ds(pl.multiple_of(zz * width, width), width)
            chosen, taken = hits(zz * width, width)
            rhs_out[start, hd:] = chosen.astype(jnp.bfloat16)
            keep[start, :] = jnp.broadcast_to(1.0 - taken, (width, hd)).astype(jnp.bfloat16)

        lhs_out[:, :hd] = qb[0].reshape(group * tok, hd)

    def k_copy(i, source, target, rows, to):
        return remote(kb.at[source, 0, rows], kb.at[target, 0, rows], sent.at[0], krecv.at[i], to)

    def b_copy(i, dz, rows, to):
        ref = bb.at[lax.rem(z + dz + nz, nz), xc, rows]
        return remote(ref, ref, sent.at[1], come.at[5], to)

    rows_k, rows_b = pl.ds(0, BLK), pl.ds(0, held)
    key_z = {d: k_copy(d, 0, d, rows_k, dev(z + d, x, c)) for d in direct}
    bank_z = {d: b_copy(0, 0, rows_b, dev(z + d, x, c)) for d in range(1, nz)}
    relays = {}
    if nz == 8:
        up, down = (1, 2), (7, 6)
        for i, source, target, part, parts_of, to in (
            (3, 2, 3, 0, 1, up[0]), (5, 6, 5, 0, 1, down[0]),
            (4, 2, 4, 0, 2, up[1]), (8, 6, 4, 1, 2, down[1]),
        ):
            rk = pl.ds(part * BLK // parts_of, BLK // parts_of)
            key_z[i] = k_copy(i, source, target, rk, dev(z + to, x, c))
            relays.setdefault(source, []).append(i)

    near = [0, 1, nz - 1, 2][:per]
    key_core = {d: remote(kb.at[d, 0], kb.at[d, 1], sent.at[2], come.at[3 if d in near else 4], sibling) for d in range(nz)}
    lo, hi = pl.ds(0, HEAD_CUT), pl.ds(HEAD_CUT, group - HEAD_CUT)

    def q_copy(i, src_slot, dst_slot, heads, target):
        return remote(qb.at[src_slot, heads], qb.at[dst_slot, heads], qsend.at[i], qrecv.at[i], target)

    q_x = [
        q_copy(0, 0, 1, lo, east), q_copy(1, 0, 1, hi, east),
        q_copy(2, 0, 3, hi, west), q_copy(3, 0, 3, lo, west),
        q_copy(4, 1, 2, lo, east), q_copy(5, 3, 2, hi, west),
    ]
    first, last = pl.ds(0, half_z), pl.ds(half_z, half_z)

    def c_copy(i, column, rows, target):
        return remote(bb.at[rows, column], bb.at[rows, column], sent.at[3], cr.at[i], target)

    def column(dx):
        return lax.rem(x + dx, NX) * 2 + c

    west_of, east_of = column(NX - 1), column(1)
    bank_x = [
        c_copy(0, xc, first, east), c_copy(1, xc, last, east),
        c_copy(2, xc, last, west), c_copy(3, xc, first, west),
        c_copy(4, west_of, first, east), c_copy(5, east_of, last, west),
    ]
    bank_in = [
        c_copy(0, west_of, first, east), c_copy(1, west_of, last, east),
        c_copy(2, east_of, last, west), c_copy(3, east_of, first, west),
        c_copy(4, column(2), first, east), c_copy(5, column(2), last, west),
    ]

    def e_copy(dx):
        return remote(bb.at[:, column(dx)], bb.at[:, column(dx)], sent.at[4], come.at[0], sibling)

    bank_core = [e_copy(dx) for dx in range(NX)]

    def together(ref, i, j=0):
        return remote(ref, ref, sent.at[i], come.at[j], sibling)

    all_keys = together(kb.at[pl.ds(0, nz - 1), 0], 0)
    all_shards = together(bb.at[pl.ds(0, nz - 1), 0], 1)
    all_key_core = together(kb.at[:, 0], 2)
    all_bank_x = together(bb.at[:, pl.ds(0, 3)], 3)
    all_bank_core = together(bb.at[:, pl.ds(0, NX)], 4, 0)
    all_parts = together(rb.at[pl.ds(1, 2 * nz - 1)], 5, 1)
    all_sums = together(rx.at[pl.ds(0, (2 * NX - 1) * nz)], 6, 2)
    near_keys = together(kb.at[pl.ds(0, per), 1], 2, 3)
    far_keys = together(kb.at[pl.ds(0, nz - per), 1], 2, 4) if groups > 1 else None
    rest_shards = together(bb.at[pl.ds(0, nz - 1), 0], 1, 5)

    def start_all():
        own[0].wait()
        for d in direct:
            key_z[d].start()
        key_core[0].start()
        own[1].wait()
        q_x[0].start()
        q_x[3].start()
        own[4].wait()
        prepare()

    def second_part():
        q_x[0].wait_send()
        q_x[1].start()
        q_x[3].wait_send()
        q_x[2].start()

    def pass_key(d):
        key_z[d].wait_recv()
        if d == 4 and nz == 8:
            key_z[8].wait_recv()
        for i in relays.get(d, ()):
            key_z[i].start()
        key_core[d].start()

    def bank_rows():
        rest_shards.wait_recv()
        for i in (0, 2, 1, 3):
            bank_x[i].start()
        bank_core[0].start()

    def bank_forward():
        bank_in[0].wait_recv()
        bank_x[4].start()
        bank_in[2].wait_recv()
        bank_x[5].start()

    def bank_cross():
        bank_in[1].wait_recv()
        bank_core[3].start()
        bank_in[3].wait_recv()
        bank_core[1].start()

    def before(pair, g, part=0):
        if (pair, g, part) == (0, 0, 0):
            start_all()
            second_part()
            for d in direct[:2]:
                pass_key(d)
            for d in direct[2:]:
                pass_key(d)
            q_x[0].wait_recv()
            q_x[4].start()
            near_keys.wait_recv()
            own[2].wait()
            for d in direct:
                bank_z[d].start()
            q_x[3].wait_recv()
        if (pair, g, part) == (0, 0, 1):
            q_x[2].wait_recv()
            q_x[5].start()
            for d in (3, 5, 4) if nz == 8 else ():
                pass_key(d)
            for d in range(1, nz):
                if d not in direct:
                    bank_z[d].start()
            q_x[1].wait_recv()
        if (pair, g) == (0, 1):
            far_keys.wait_recv()
        if (pair, g) == (1, 0):
            q_x[4].wait_recv()
            q_x[5].wait_recv()
            if groups == 1:
                bank_rows()
        if groups > 1 and (pair, g) == (1, groups - 1):
            bank_rows()

    lane = lax.broadcasted_iota(jnp.int32, (1, BLK), 1)

    def compute(pair, g, heads):
        tiles = (1 - pair, 3 - pair)
        offsets = near if groups == 1 else [6 * g, 1 + 2 * g, 7 - 2 * g, 2 + 2 * g]
        members = [(d, rel) for d in offsets for rel in range(2)]
        keys = jnp.concatenate([kb[d].reshape(2 * BLK, hd) for d in offsets], axis=0)
        position = [(z * 2 * NX + lax.rem(x - t + NX, NX) * 2 + c) * tok + lane for t in tiles]
        first_in, any_in = [], []
        for d, rel in members:
            begin = ws[(lax.rem(z - d + nz, nz) * NX + x) * 2 + (c + rel) % 2]
            hit = [(p >= begin) & (p < begin + WIN) for p in position]
            first_in.append(hit[0])
            any_in.append((hit[0] | hit[1]).astype(jnp.float32))
        sums = [acc[d, rel] for d, rel in members]
        for h in heads:
            rows = jnp.concatenate([qb[t, h] for t in tiles], axis=0)
            scores = lax.dot_general(
                keys, rows, (((1,), (1,)), ((), ())), preferred_element_type=jnp.float32
            )
            for i in range(len(members)):
                both = scores[i * BLK : (i + 1) * BLK]
                part_scores = jnp.where(first_in[i], both[:, :tok], both[:, tok:])
                top = jnp.max(part_scores, axis=0, keepdims=True)
                e = jnp.exp2((part_scores - top) * exp_scale)
                sums[i] = sums[i] + e * (any_in[i] / jnp.sum(e, axis=0, keepdims=True))
        for (d, rel), value in zip(members, sums):
            acc[d, rel] = value

    before(0, 0, 0)
    compute(0, 0, range(HEAD_CUT))
    before(0, 0, 1)
    compute(0, 0, range(HEAD_CUT, group))

    for k in range(1, 2 * groups - 1):
        before(k // groups, k % groups)
        compute(k // groups, k % groups, range(group))

    def partial(offsets):
        for d in offsets:
            for rel in range(2):
                weight = jnp.sum(acc[d, rel], axis=1, keepdims=True)
                row = jnp.sum(weight * kb[d, rel].astype(jnp.float32), axis=0, keepdims=True)
                pb[(c + rel) % 2, pl.ds(lax.rem(z - d + nz, nz), 1), :] = row

    before(1, groups - 1)
    compute(1, groups - 1, range(group))
    if groups > 1:
        partial(near)
    partial([d for d in range(nz) if groups == 1 or d not in near])

    column_peers = [(dz, dc) for dz in range(nz) for dc in range(2) if dz or dc]
    column_peers.sort(key=lambda p: -min(p[0], nz - p[0]))
    parts = [
        remote(pb.at[(c + dc) % 2], rb.at[dz * 2 + dc], sent.at[5], come.at[1], dev(z + dz, x, (c + dc) % 2))
        for dz, dc in column_peers
    ]
    for copy in parts:
        copy.start()
    rb[0] = pb[c]
    bank_forward()
    bank_cross()
    all_parts.wait_recv()
    total = jnp.zeros((nz, hd), jnp.float32)
    for dz in range(nz):
        for dc in range(2):
            total = total + rb[lax.rem(z - dz + nz, nz) * 2 + (c + dc) % 2]
    mine = pl.ds(pl.multiple_of(xc * nz, nz), nz)
    rx[mine, :] = total / (group * WIN)
    row_peers = [(dx, dc) for dx in range(NX) for dc in range(2) if dx or dc]
    row_peers.sort(key=lambda p: -min(p[0], NX - p[0]))
    sums_x = [
        remote(rx.at[mine], rx.at[mine], sent.at[6], come.at[2], dev(z, x + dx, (c + dc) % 2))
        for dx, dc in row_peers
    ]
    for copy in sums_x:
        copy.start()
    bank_in[4].wait_recv()
    bank_in[5].wait_recv()
    bank_core[2].start()
    for copy in (all_keys, all_shards, all_key_core, all_bank_x, all_parts, q_x[1], q_x[2], q_x[4], q_x[5]):
        copy.wait_send()
    all_bank_core.wait()

    @pl.loop(0, nz)
    def _(zz):
        start = pl.ds(pl.multiple_of(zz * width, width), width)
        rhs_out[start, :hd] = bb[zz].reshape(width, hd) * keep[start, :]

    chosen, taken = hits(s * held, held)
    all_sums.wait_recv()
    ordered = [rx[pl.ds(zz, 2 * NX, stride=nz), :] for zz in range(nz)]
    reps = jnp.concatenate(ordered, axis=0).astype(jnp.bfloat16)
    value = lax.dot_general(
        lhs_out[:, :hd], jnp.concatenate([reps, reps], axis=0), (((1,), (1,)), ((), ())),
        preferred_element_type=jnp.float32,
    )
    high = value.astype(jnp.bfloat16).astype(jnp.float32)
    left = lax.broadcasted_iota(jnp.int32, (1, 2 * reps.shape[0]), 1) < reps.shape[0]
    lhs_out[:, hd:] = jnp.where(left, high, value - high).astype(jnp.bfloat16)
    placed = jnp.dot(
        chosen[:, : reps.shape[0]].astype(jnp.bfloat16), reps, preferred_element_type=jnp.float32
    )
    shard_out[...] = jnp.where(taken > 0.5, placed, bb[z, xc].astype(jnp.float32)).astype(jnp.bfloat16)
    all_sums.wait_send()


def refresh(nz, window_start, slots, q, k, b):
    group, tok, hd = q.shape
    hbm = pl.BlockSpec(memory_space=pl.ANY)
    vmem = pl.BlockSpec(memory_space=VMEM)
    dma = pltpu.SemaphoreType.DMA
    bank_shape = (nz, 2 * NX, *b.shape)
    return pl.pallas_call(
        functools.partial(refresh_kernel, nz),
        out_shape=(
            on_chip((nz * 2 * NX * b.shape[0], hd + 2 * slots.shape[1]), jnp.bfloat16),
            on_chip((group * tok, hd + 2 * slots.shape[1]), jnp.bfloat16),
            on_chip(b.shape, jnp.bfloat16),
        ),
        in_specs=[hbm] * 5,
        out_specs=(vmem, vmem, vmem),
        scratch_shapes=[
            pltpu.SMEM(window_start.shape, jnp.int32),
            VMEM(slots.shape, jnp.int32),
            VMEM((NX, group, tok, hd), jnp.bfloat16),
            VMEM((nz, 2, BLK, hd), jnp.bfloat16),
            VMEM(bank_shape, jnp.bfloat16),
            VMEM((nz * 2 * NX * b.shape[0], hd), jnp.bfloat16),
            VMEM((nz, 2, BLK, BLK), jnp.float32),
            VMEM((2, nz, hd), jnp.float32),
            VMEM((2 * nz, nz, hd), jnp.float32),
            VMEM((2 * NX * nz, hd), jnp.float32),
            dma((5,)), dma((7,)), dma((6,)),
            dma((nz + 1,)), dma((6,)), dma((6,)), dma((6,)),
        ],
        compiler_params=pltpu.CompilerParams(collective_id=0, has_side_effects=True),
        name="refresh",
    )(window_start, slots, q, k, b)


def relevance_kernel(tile, lhs, rhs, shard, out, shard_out, held, sem):
    scale = 1.0 / math.sqrt(BLK)
    copies = [pltpu.make_async_copy(shard, shard_out, sem.at[0])]
    copies[0].start()
    for i in range(out.shape[1] // tile):
        cut = pl.ds(i * tile, tile)
        scores = lax.dot_general(
            lhs[...], rhs[cut, :], (((1,), (1,)), ((), ())), preferred_element_type=jnp.float32
        )
        held[:, cut] = (scores * scale).astype(jnp.bfloat16)
        copy = pltpu.make_async_copy(held.at[:, cut], out.at[:, cut], sem.at[i + 1])
        copy.start()
        copies.append(copy)
    for copy in copies:
        copy.wait()


def relevance_of(lhs, rhs, shard, tile=512):
    rows, total = lhs.shape[0], rhs.shape[0]
    vmem = pl.BlockSpec(memory_space=VMEM)
    hbm = pl.BlockSpec(memory_space=pl.ANY)
    lhs, rhs, shard = (kept(a) for a in (lhs, rhs, shard))
    return pl.pallas_call(
        functools.partial(relevance_kernel, tile),
        out_shape=(
            jax.ShapeDtypeStruct((rows, total), jnp.bfloat16),
            jax.ShapeDtypeStruct(shard.shape, jnp.bfloat16),
        ),
        in_specs=[vmem, vmem, vmem],
        out_specs=(hbm, hbm),
        scratch_shapes=[
            VMEM((rows, total), jnp.bfloat16),
            pltpu.SemaphoreType.DMA((1 + total // tile,)),
        ],
        name="relevance",
    )(lhs, rhs, shard)


def per_device(nz, queries, new_keys, cache_keys, window_start, owner_slot):
    tok, group, hd = queries.shape
    q = queries.transpose(1, 0, 2)
    rhs, lhs, shard = refresh(
        nz, window_start, owner_slot.reshape(1, -1), q, new_keys[:, 0, :], cache_keys[:, 0, :]
    )
    relevance, new_shard = relevance_of(lhs, rhs, shard)
    relevance = relevance.reshape(group, tok, rhs.shape[0]).transpose(1, 0, 2)
    return (relevance, new_shard[:, None, :])


def solution(mesh):
    nz = mesh.shape["seq"] // (2 * NX)
    split = P("seq", "kvh", None)
    return jax.shard_map(
        functools.partial(per_device, nz),
        mesh=mesh,
        in_specs=(split, split, split, P(), P()),
        out_specs=(split, split),
        check_vma=False,
    )
```
